32 devices in a mesh: seq: 4 (over z), nbr: 4 (over y, x), batch: 2 (over core).
Axes of the slice: x: 2, y: 2, z: 4, core: 2. Of those that a mesh axis runs over, the one named last changes fastest.
Arguments:
- hidden: bfloat16 [1024, 4096], P(('batch', 'seq'), 'nbr'), parts along dimension 0, may hold values from -6 to 6
- d_out: bfloat16 [1024, 4096], P(('batch', 'seq'), 'nbr'), parts along dimension 0, may hold values from -6 to 6
- nbr_emb: bfloat16 [192, 128, 896], P(('batch', 'seq', 'nbr')), parts along dimension 0, may hold values from -6 to 6
- slot_span: int32 [192], P(('batch', 'seq')), parts along dimension 0, may hold values from -1 to 1, as said below
- dec_gain: bfloat16 [4096], P('nbr'), may hold values from 0.5 to 1.5
- enc_gain: bfloat16 [896], replicated, may hold values from 0.5 to 1.5
- w_cond: bfloat16 [4096, 896], P('nbr'), may hold values from -0.75 to 0.75
- w_enc: bfloat16 [896, 896], replicated, may hold values from -0.1875 to 0.1875
- w_q: bfloat16 [4096, 2048], P('seq', 'nbr'), may hold values from -0.09375 to 0.09375
- w_k: bfloat16 [896, 2048], P('seq', 'nbr'), may hold values from -8 to 8
- w_v: bfloat16 [896, 2048], P('seq', 'nbr'), may hold values from -0.1875 to 0.1875
- w_o: bfloat16 [2048, 4096], P('nbr', 'seq'), may hold values from -0.125 to 0.125
Outputs:
- out: bfloat16 [1024, 4096], P(('batch', 'seq'), 'nbr'), parts along dimension 0
- d_hidden: bfloat16 [1024, 4096], P(('batch', 'seq'), 'nbr'), parts along dimension 0
- d_enc: bfloat16 [192, 128, 896], P(('batch', 'seq', 'nbr')), parts along dimension 0
- d_wo: float32 [4096, 4096], P(('batch', 'nbr'), 'seq'), parts along dimension 0
- d_wk: float32 [1792, 2048], P(('batch', 'seq'), 'nbr'), parts along dimension 0
- d_wv: float32 [1792, 2048], P(('batch', 'seq'), 'nbr'), parts along dimension 0
The draws below stay inside these ranges and needn't reach their ends.
There are 2 independent parts, one for each index of `batch`. The reference program is written for one: setup_inputs(seed, part) draws one part's arguments, and reference() takes and returns one part's arrays. A program takes and returns all parts, laid end to end along the dimension named above; an argument that names none is the same for every part. Nothing has to cross between parts.
Inputs may be any that keep to these rules, and one draw needn't show every extreme that they name: `slot_span`: A slot on seq index s serves a span of seq index s, counted from 0 within its 2 spans; -1 marks an empty slot. Every span is served by 1 to 8 slots, and one span of each seq index by exactly 8. Within each seq index one nbr index has all 6 slots live.
All inputs are finite; a program needn't handle non-finite values.
Results may differ from the reference program's by a relative error of at most 0.018.
The reference program's roundings to bfloat16 on the way count: a program that leaves them out, or rounds other values in their place, can miss the bound.
Values may be sent and summed in bfloat16 or wider, within the bound.
A program may use at most 128 MiB of HBM per device.

```python
import jax
import jax.numpy as jnp
from jax import lax

D = 4096
EW = 896
H = 16
HD = 128
CLEN = 64
NLEN = 128
KMAX = 8
NEIGHBOUR_SLOTS = 6
TOK_DEV = 128
TOKENS = 512
SPANS_PER_INDEX = 2
SPANS = 8
GSLOT = 24
SLOTS = 96
HW = 2048
N_SEQ = 4
N_NBR = 4


def draw_group_index(group_random_key):
    slot_count = NEIGHBOUR_SLOTS * N_NBR
    batch_random_key, occupy_random_key, order_random_key, first_random_key = jax.random.split(group_random_key, 4)
    draw_batch = jax.random.randint(batch_random_key, (), 0, SPANS_PER_INDEX)
    span_index = jnp.arange(slot_count, dtype=jnp.int32)
    remaining_slots = span_index - SPANS_PER_INDEX - KMAX + 1
    other_device = (draw_batch + 1 + remaining_slots % (SPANS_PER_INDEX - 1)) % SPANS_PER_INDEX
    occupied_slots = (jax.random.randint(occupy_random_key, (slot_count,), 0, 4) == 0) & (remaining_slots < (KMAX - 1) * (SPANS_PER_INDEX - 1))
    group_label = jnp.where(span_index < SPANS_PER_INDEX, span_index, jnp.where(remaining_slots < 0, draw_batch, jnp.where(occupied_slots, other_device, -1)))
    group_label = group_label.astype(jnp.int32)
    shuffle = jax.random.permutation(order_random_key, slot_count).astype(jnp.int32)
    ranked = jnp.where(group_label >= 0, 0, slot_count) + shuffle
    order = jnp.argsort(ranked)
    ordered = group_label[order]
    first_slot = jax.random.randint(first_random_key, (), 0, N_NBR)
    device_index = (span_index // NEIGHBOUR_SLOTS + first_slot) % N_NBR
    target_device = (device_index * NEIGHBOUR_SLOTS + span_index % NEIGHBOUR_SLOTS).astype(jnp.int32)
    return jnp.zeros((slot_count,), jnp.int32).at[target_device].set(ordered)


def draw_slot_span(key, part):
    group_key_list = jax.random.split(jax.random.fold_in(key, 17), N_SEQ)
    return jax.vmap(draw_group_index)(group_key_list).reshape(N_SEQ * NEIGHBOUR_SLOTS * N_NBR)


def draw_w_k(key, part):
    k_base, k_heads = jax.random.split(jax.random.fold_in(key, 29))
    base = jnp.clip(jax.random.normal(k_base, (EW, HW), jnp.float32), -4.0, 4.0) * EW ** (-0.5)
    picked = jax.random.permutation(k_heads, H)
    column_head = jnp.arange(HW, dtype=jnp.int32) // HD
    strength = jnp.where(column_head == picked[0], 2.5, 1.0)
    return jnp.clip(base * strength[None, :].astype(jnp.float32), -8.0, 8.0).astype(jnp.bfloat16)


def steps_of(own_key, dims, cuts, least, high):
    def one(dim, parts):
        draws = jax.random.uniform(jax.random.fold_in(jax.random.fold_in(own_key, 6), dim), (parts,), jnp.float32, least / len(cuts), high / len(cuts))
        return jnp.repeat(jnp.exp(draws), dims[dim] // parts).reshape((-1,) + (1,) * (len(dims) - dim - 1))

    factor_of = one(*cuts[0])
    for cut in cuts[1:]:
        factor_of = factor_of * one(*cut)
    return factor_of


def bell_draw(rng, dims, scale, bound, shards=(), kind=jnp.bfloat16):
    result = jax.random.normal(rng, dims, jnp.float32) * scale
    if len(shards) > 0:
        result = steps_of(rng, dims, shards, -0.22, 0.18) * result
    return jnp.clip(result, min=-bound, max=bound).astype(kind)


def setup_inputs(seed: int = 0, part: int = 0) -> dict:
    key_list = jax.random.split(jax.random.key(seed), 13)
    part_splits = jax.random.split(jax.random.fold_in(key_list[12], part), 13)
    hidden = bell_draw(part_splits[0], (TOKENS, D), 1.0, 6.0, ((0, 4), (1, 4)))
    d_out = bell_draw(part_splits[1], (TOKENS, D), 1.0, 6.0, ((0, 4), (1, 4)))
    nbr_emb = bell_draw(part_splits[2], (SLOTS, NLEN, EW), 1.0, 6.0, ((0, 16),))
    slot_span = draw_slot_span(jax.random.fold_in(jax.random.fold_in(key_list[12], part), 71), part)
    dec_gain = jnp.clip(1.0 + 0.1 * jax.random.normal(key_list[4], (D,), jnp.float32), 0.5, 1.5).astype(jnp.bfloat16)
    enc_gain = jnp.clip(1.0 + 0.1 * jax.random.normal(key_list[5], (EW,), jnp.float32), 0.5, 1.5).astype(jnp.bfloat16)
    w_cond = bell_draw(key_list[6], (D, EW), (D // 64) ** -0.5, 0.75, ((0, 4),))
    w_enc = bell_draw(key_list[7], (EW, EW), EW ** -0.5, 0.1875)
    w_q = bell_draw(key_list[8], (D, HW), D ** -0.5, 0.09375, ((0, 4), (1, 4)))
    w_k = draw_w_k(jax.random.fold_in(key_list[12], 71), part)
    w_v = bell_draw(key_list[10], (EW, HW), EW ** -0.5, 0.1875, ((0, 4), (1, 4)))
    w_o = bell_draw(key_list[11], (HW, D), HW ** -0.5, 0.125, ((0, 4), (1, 4)))
    return dict(hidden=hidden, d_out=d_out, nbr_emb=nbr_emb, slot_span=slot_span, dec_gain=dec_gain, enc_gain=enc_gain, w_cond=w_cond, w_enc=w_enc, w_q=w_q, w_k=w_k, w_v=w_v, w_o=w_o)


def rms_scale(values):
    return lax.rsqrt(lax.optimization_barrier(jnp.mean(values * values, axis=-1, keepdims=True)) + 1e-06)

def group_attention(operands):
    query, keys, values, d_attn, owners = operands
    factor = HD ** (-0.5)
    token_span = jnp.arange(TOK_DEV, dtype=jnp.int32) // CLEN
    key_span = jnp.repeat(owners, NLEN)
    allowed = token_span[:, None] == key_span[None, :]
    qf = query.astype(jnp.float32)
    kf = keys.astype(jnp.float32)
    vf = values.astype(jnp.float32)
    df = d_attn.astype(jnp.float32)
    scores = jnp.einsum('thd,khd->htk', qf, kf) * factor
    scores = jnp.where(allowed[None], scores, -1e+30)
    peak = lax.optimization_barrier(jnp.max(scores, axis=-1, keepdims=True))
    weights = jnp.exp(scores - peak)
    probs = weights / lax.optimization_barrier(jnp.sum(weights, axis=-1, keepdims=True))
    probs_b = probs.astype(jnp.bfloat16)
    pf = probs_b.astype(jnp.float32)
    attended = jnp.einsum('htk,khd->thd', pf, vf).astype(jnp.bfloat16)
    d_probs = jnp.einsum('thd,khd->htk', df, vf)
    row_dot = lax.optimization_barrier(jnp.sum(probs * d_probs, axis=-1, keepdims=True))
    d_scores = (probs * (d_probs - row_dot) * factor).astype(jnp.bfloat16).astype(jnp.float32)
    d_query = jnp.einsum('htk,khd->thd', d_scores, kf).astype(jnp.bfloat16)
    d_key = jnp.einsum('htk,thd->khd', d_scores, qf).astype(jnp.bfloat16)
    d_value = jnp.einsum('htk,thd->khd', pf, df).astype(jnp.bfloat16)
    return (attended, d_query, d_key, d_value)

def reference(hidden, d_out, nbr_emb, slot_span, dec_gain, enc_gain, w_cond, w_enc, w_q, w_k, w_v, w_o):
    hf = hidden.astype(jnp.float32)
    pooled = lax.optimization_barrier(jnp.mean(hf.reshape(SPANS, CLEN, D), axis=1)).astype(jnp.bfloat16)
    before = jnp.concatenate([jnp.zeros((1, D), jnp.bfloat16), pooled[:SPANS - 1]], axis=0)
    cond = jnp.dot(before, w_cond, preferred_element_type=jnp.float32)
    group_index = jnp.arange(SLOTS, dtype=jnp.int32) // GSLOT
    live = slot_span >= 0
    served = (group_index * SPANS_PER_INDEX + jnp.maximum(slot_span, 0)).astype(jnp.int32)
    slot_cond = jnp.where(live[:, None], cond[served], jnp.float32(0.0))
    inputs = nbr_emb.astype(jnp.float32) + slot_cond[:, None, :]
    enc_normed = (inputs * rms_scale(inputs) * enc_gain.astype(jnp.float32)).astype(jnp.bfloat16)
    mixed = jnp.dot(enc_normed.reshape(-1, EW), w_enc, preferred_element_type=jnp.float32).reshape(inputs.shape)
    encoded = (inputs + jax.nn.silu(mixed)).astype(jnp.bfloat16)
    enc_rows = encoded.reshape(-1, EW)
    rstd = rms_scale(hf)
    normed = (hf * rstd * dec_gain.astype(jnp.float32)).astype(jnp.bfloat16)
    query = jnp.dot(normed, w_q, preferred_element_type=jnp.float32).astype(jnp.bfloat16)
    keys = jnp.dot(enc_rows, w_k, preferred_element_type=jnp.float32).astype(jnp.bfloat16)
    values = jnp.dot(enc_rows, w_v, preferred_element_type=jnp.float32).astype(jnp.bfloat16)
    d_attn = jnp.dot(d_out, w_o.T, preferred_element_type=jnp.float32).astype(jnp.bfloat16)
    attended, d_query, d_key, d_value = lax.map(group_attention, (query.reshape(N_SEQ, TOK_DEV, H, HD), keys.reshape(N_SEQ, GSLOT * NLEN, H, HD), values.reshape(N_SEQ, GSLOT * NLEN, H, HD), d_attn.reshape(N_SEQ, TOK_DEV, H, HD), slot_span.reshape(N_SEQ, GSLOT)))
    attended = attended.reshape(TOKENS, HW)
    d_query = d_query.reshape(TOKENS, HW)
    d_key = d_key.reshape(SLOTS * NLEN, HW)
    d_value = d_value.reshape(SLOTS * NLEN, HW)
    out = (hf + jnp.dot(attended, w_o, preferred_element_type=jnp.float32)).astype(jnp.bfloat16)
    d_wo = jnp.dot(attended.T, d_out, preferred_element_type=jnp.float32)
    d_wk = jnp.dot(enc_rows.T, d_key, preferred_element_type=jnp.float32)
    d_wv = jnp.dot(enc_rows.T, d_value, preferred_element_type=jnp.float32)
    block = HW // N_NBR
    total = jnp.zeros((SLOTS * NLEN, EW), jnp.float32)
    for span_index in range(N_NBR):
        lower = span_index * block
        upper = lower + block
        part = jnp.dot(d_key[:, lower:upper], w_k[:, lower:upper].T, preferred_element_type=jnp.float32)
        part = part + jnp.dot(d_value[:, lower:upper], w_v[:, lower:upper].T, preferred_element_type=jnp.float32)
        total = total + part.astype(jnp.bfloat16).astype(jnp.float32)
    d_enc = total.reshape(SLOTS, NLEN, EW).astype(jnp.bfloat16)
    d_normed = jnp.dot(d_query, w_q.T, preferred_element_type=jnp.float32)
    scaled_grad = dec_gain.astype(jnp.float32) * d_normed
    stat = lax.optimization_barrier(jnp.mean(hf * scaled_grad, axis=-1, keepdims=True))
    d_hidden = (d_out.astype(jnp.float32) + rstd * scaled_grad - hf * rstd ** 3 * stat).astype(jnp.bfloat16)
    return (out, d_hidden, d_enc, d_wo, d_wk, d_wv)
```

```python
import functools

import jax
import jax.numpy as jnp
from jax import lax
from jax.experimental import pallas as pl
from jax.experimental.pallas import tpu as pltpu
from jax.sharding import PartitionSpec as P

HD = 128
CLEN = 64
NLEN = 128
KMAX = 8
BF = jnp.bfloat16
F32 = jnp.float32
MESH = pl.DeviceIdType.MESH
ANY = pl.BlockSpec(memory_space=pl.ANY)
NT = (((1,), (1,)), ((), ()))
TN = (((0,), (0,)), ((), ()))
TILE = 256

dot = functools.partial(lax.dot_general, preferred_element_type=F32)


def mm(a, b):
    return jnp.dot(a, b, preferred_element_type=F32)


def remote(src, dst, send, recv, dev):
    return pltpu.make_async_remote_copy(
        src_ref=src, dst_ref=dst, send_sem=send, recv_sem=recv, device_id=dev, device_id_type=MESH
    )


def cols(ref, i, width):
    return ref.at[:, pl.ds(pl.multiple_of(i * width, 128), width)]


def rows_of(ref, i, count):
    return ref.at[pl.ds(pl.multiple_of(i * count, 8), count)]


def tiles(count, step, body):
    def one(t, _):
        body(pl.multiple_of(t * step, step))
        return 0

    lax.fori_loop(0, count // step, one, 0)


def layer_kernel(n_seq, n_nbr, names, *refs):
    hidden, d_out, gain, emb, span, e_gain, w_cond, w_enc, w_q, w_k, w_v, w_o = refs[:12]
    out_o, dh_o, denc_o, dwo_o, dwk_o, dwv_o = refs[12:18]
    S = dict(zip(names, refs[18:]))
    hid, dout, gains, wq, wo, wkv = (S[k] for k in ("hid", "dout", "gains", "wq", "wo", "wkv"))
    enc, enct, kv, big, norm, rst = (S[k] for k in ("enc", "enct", "kv", "big", "norm", "rst"))
    e1, e2, e3, po, pd = (S[k] for k in ("e1", "e2", "e3", "po", "pd"))
    ro, rd, q_s, da_s, dq_s = (S[k] for k in ("ro", "rd", "q", "da", "dq"))
    att, dcol, pw, wr, dwo, dwf = (S[k] for k in ("att", "dcol", "pw", "wr", "dwo", "dwf"))
    emb_v, cond_v, enc_v, pool = (S[k] for k in ("emb", "cond", "wenc", "pool"))
    cpart, crecv, st = (S[k] for k in ("cpart", "crecv", "st"))
    lsem, osem, zs, zr, ps, pr = (S[k] for k in ("lsem", "osem", "zs", "zr", "ps", "pr"))
    ns, nr, es, er, ss, sr = (S[k] for k in ("ns", "nr", "es", "er", "ss", "sr"))
    us, ur, ks, kr = (S[k] for k in ("us", "ur", "ks", "kr"))

    s, n, b = lax.axis_index("seq"), lax.axis_index("nbr"), lax.axis_index("batch")
    x, y, core, diag = {"nbr": n ^ 1}, {"nbr": n ^ 2}, {"batch": 1 - b}, {"nbr": n ^ 3}
    right, left = {"seq": s + 1}, {"seq": s - 1}
    has_right, has_left = s + 1 < n_seq, s > 0
    tokens, feat = hidden.shape
    spans = tokens // CLEN
    slots, width = emb.shape[0], emb.shape[2]
    total = slots * n_nbr
    local = w_q.shape[1]
    heads = local // HD
    half_slots = slots // 2
    unit = half_slots * NLEN
    wr_q, wr_k, piece = w_q.shape[0], w_k.shape[0], w_o.shape[1]

    own = {
        "h": cols(hid, n, feat), "d": cols(dout, n, feat), "g": gains.at[n],
        "k": rows_of(wkv, s, wr_k).at[:, pl.ds(0, local)],
        "v": rows_of(wkv, s, wr_k).at[:, pl.ds(local, local)],
        "q": rows_of(wq, s, wr_q), "o": cols(wo, s, piece),
    }
    source = {"h": hidden, "d": d_out, "g": gain, "k": w_k, "v": w_v, "q": w_q, "o": w_o}
    loads = {
        k: pltpu.make_async_copy(source[k], own[k], lsem.at[i]) for i, k in enumerate(("h", "d", "g", "k", "v", "q", "o"))
    }
    loads["c"] = pltpu.make_async_copy(w_cond, cond_v, lsem.at[7])
    loads["e"] = pltpu.make_async_copy(emb, emb_v, lsem.at[8])
    loads["w"] = pltpu.make_async_copy(w_enc, enc_v, lsem.at[9])
    for k in ("h", "k", "v", "q", "g", "c", "d", "e", "w", "o"):
        loads[k].start()

    barrier = pltpu.get_barrier_semaphore()
    for dev in (x, y, diag, core):
        pl.semaphore_signal(barrier, inc=1, device_id=dev, device_id_type=MESH)
    for k in range(1, n_seq):
        pl.semaphore_signal(barrier, inc=1, device_id={"seq": lax.rem(s + k, n_seq)}, device_id_type=MESH)

    loads["h"].wait()
    means = []
    for c in range(spans):
        part = cols(hid, n, feat)[c * CLEN : (c + 1) * CLEN, :].astype(F32)
        means.append((jnp.sum(part, axis=0, keepdims=True) / CLEN).astype(BF).astype(F32))
    pool[0] = jnp.broadcast_to(means[spans - 1], pool.shape[1:])
    pl.semaphore_wait(barrier, n_seq + 3)

    def carry(dev):
        return remote(pool.at[0], pool.at[1], ss.at[0], sr.at[0], dev)

    @pl.when(has_right)
    def _():
        carry(right).start()

    order = ("k", "v", "q", "o")

    def block(a, j):
        if a == "k":
            return rows_of(wkv, j, wr_k).at[:, pl.ds(0, local)]
        if a == "v":
            return rows_of(wkv, j, wr_k).at[:, pl.ds(local, local)]
        if a == "q":
            return rows_of(wq, j, wr_q)
        return cols(wo, j, piece)

    def half(a, j, h):
        if a in ("k", "v"):
            w = local // 2
            base = 0 if a == "k" else local
            return rows_of(wkv, j, wr_k).at[:, pl.ds(pl.multiple_of(base + h * w, 128), w)]
        if a == "q":
            c = wr_q // 2
            return wq.at[pl.ds(pl.multiple_of(j * wr_q + h * c, 8), c)]
        c = local // 2
        return wo.at[pl.ds(pl.multiple_of(h * c, 8), c), pl.ds(pl.multiple_of(j * piece, 128), piece)]

    def ring(a, k, d):
        j = s - k + 1 if d == 0 else s + k - 1
        i = order.index(a)
        part = half(a, j, b)
        return remote(part, part, zs.at[i, k, d], zr.at[i, k, d], right if d == 0 else left)

    def guard(d, k):
        if d == 0:
            return has_right & (s - (k - 1) >= 0)
        return has_left & (s + (k - 1) < n_seq)

    def valid(d, k):
        return (s - k >= 0) if d == 0 else (s + k < n_seq)

    def launch(a):
        loads[a].wait()
        for d in (0, 1):
            @pl.when(guard(d, 1))
            def _(a=a, d=d):
                ring(a, 1, d).start()

    def share(a, k, d, h):
        j = s - k if d == 0 else s + k
        i = order.index(a)
        part = half(a, j, h)
        return remote(part, part, ps.at[i, k, d], pr.at[i, k, d], core)

    def relay(a, k):
        i = order.index(a)
        for d in (0, 1):
            @pl.when(valid(d, k))
            def _(d=d):
                part = half(a, s - k if d == 0 else s + k, b)
                remote(part, part, zs.at[i, k, d], zr.at[i, k, d], left if d == 0 else right).wait_recv()
                share(a, k, d, b).start()

            if k + 1 < n_seq:
                @pl.when(guard(d, k + 1))
                def _(d=d):
                    ring(a, k + 1, d).start()

    def arrived(a):
        for k in range(1, n_seq):
            for d in (0, 1):
                @pl.when(valid(d, k))
                def _(k=k, d=d):
                    share(a, k, d, 1 - b).wait_recv()

    def wave(w, skip=()):
        for a, lag in (("k", 0), ("v", 0), ("q", 1), ("o", 2)):
            if 1 <= w - lag < n_seq and a not in skip:
                relay(a, w - lag)

    for a in ("k", "v", "q"):
        launch(a)

    def pair(key, i):
        ref = own[key]
        return [remote(ref, ref, ns.at[i, d], nr.at[i, d], dev) for d, dev in enumerate((x, y))]

    for c in pair("h", 0):
        c.start()
    loads["g"].wait()
    gain_sends = [
        remote(own["g"], own["g"], ns.at[2, d], nr.at[2, d], dev) for d, dev in enumerate((x, y, diag))
    ]
    for c in gain_sends:
        c.start()

    @pl.when(has_left)
    def _():
        carry(left).wait_recv()

    @pl.when(jnp.logical_not(has_left))
    def _():
        pool[1] = jnp.zeros(pool.shape[1:], F32)

    place = lax.broadcasted_iota(jnp.int32, pool.shape[1:], 0)
    before = pool[1]
    for c in range(1, spans):
        before = jnp.where(place == c, jnp.broadcast_to(means[c - 1], before.shape), before)
    loads["c"].wait()
    cpart[...] = mm(before.astype(BF), cond_v[...])
    sums = [remote(cpart, crecv.at[d], ss.at[1 + d], sr.at[1 + d], dev) for d, dev in enumerate((x, y, diag))]
    for c in sums:
        c.start()
    loads["d"].wait()
    for c in pair("d", 1):
        c.start()
    for c in sums:
        c.wait_recv()
    condition = cpart[...] + crecv[0] + crecv[1] + crecv[2]

    def slot_rows(m, j):
        return pl.ds(pl.multiple_of((m * slots + j) * NLEN, NLEN), NLEN)

    def slot_copy(src, j, i, dev):
        part = enc.at[slot_rows(src, j)]
        return remote(part, part, es.at[j, i], er.at[j, i], dev)

    loads["e"].wait()
    loads["w"].wait()
    gain_row = e_gain[...].astype(F32)
    for j in range(slots):
        mark = jnp.full((1, width), span[n * slots + j], jnp.int32)
        vals = emb_v[j].astype(F32)
        for c in range(spans):
            vals = vals + jnp.where(mark == c, condition[c : c + 1], 0.0)
        scale = lax.rsqrt(jnp.mean(vals * vals, axis=-1, keepdims=True) + 1e-06)
        mixed = mm((vals * scale * gain_row).astype(BF), enc_v[...])
        enc[slot_rows(n, j), :] = (vals + mixed / (1.0 + jnp.exp(-mixed))).astype(BF)
        slot_copy(n, j, 0, x).start()
        slot_copy(n, j, 1, y).start()
        if j == half_slots:
            wave(1)
            launch("o")

    def diagonal(ref, i):
        c = tokens // 2
        for d, (src, dev) in enumerate(((n ^ 1, y), (n ^ 2, x))):
            full = cols(ref, src, feat)
            remote(full, full, ns.at[i, d], nr.at[i, d], dev).wait_recv()
            part = full.at[pl.ds(d * c, c)]
            remote(part, part, ns.at[i, 2 + d], nr.at[i, 2 + d], dev).start()

    def diagonal_done(ref, i):
        c = tokens // 2
        for d in (0, 1):
            part = cols(ref, n ^ 3, feat).at[pl.ds(d * c, c)]
            remote(part, part, ns.at[i, 2 + d], nr.at[i, 2 + d], x).wait()

    def pass_on(j):
        for d, (src, dev) in enumerate(((n ^ 1, y), (n ^ 2, x))):
            slot_copy(src, j, d, dev).wait_recv()
            if j % 2 == d:
                slot_copy(src, j, 2, dev).start()

    def project(m, j):
        at = pl.multiple_of((m * slots + j) * NLEN, NLEN)
        slot = pl.ds(m * slots + j, half_slots)
        block_rows = enc[pl.ds(at, unit), :]
        enct[:, pl.ds(at, unit)] = block_rows.T

        def tile(c):
            res = mm(enc[pl.ds(at, unit), :], wkv[:, pl.ds(c, TILE)]).astype(BF)
            kv[slot, :, pl.ds(c, TILE)] = res.reshape(half_slots, NLEN, TILE)

        tiles(2 * local, TILE, tile)

    diagonal(hid, 0)
    diagonal(dout, 1)
    wave(2)
    for j in range(half_slots):
        pass_on(j)
    diagonal_done(hid, 0)
    diagonal_done(dout, 1)
    for c in gain_sends:
        c.wait_recv()

    def norm_rows(r):
        part = hid[pl.ds(r, 32), :].astype(F32)
        scale = lax.rsqrt(jnp.mean(part * part, axis=-1, keepdims=True) + 1e-06)
        rst[pl.ds(r, 32), :] = jnp.broadcast_to(scale, (32, HD))
        for m in range(n_nbr):
            vals = hid[pl.ds(r, 32), m * feat : (m + 1) * feat].astype(F32) * scale * gains[m, 0:1].astype(F32)
            norm[pl.ds(r, 32), m * feat : (m + 1) * feat] = vals.astype(BF)

    tiles(tokens, 32, norm_rows)
    wave(3)
    for w in range(4, n_seq):
        wave(w)
    for j in range(half_slots, slots):
        pass_on(j)
    arrived("k")
    arrived("v")
    for m in (n, n ^ 1, n ^ 2):
        project(m, 0)
    wave(n_seq)
    for m in (n, n ^ 1, n ^ 2):
        project(m, half_slots)
    for j in range(slots):
        slot_copy(n ^ 3, j, 2, x).wait_recv()
        if (j + 1) % half_slots == 0:
            project(n ^ 3, j + 1 - half_slots)
    arrived("q")

    def query(c):
        q_s[:, pl.ds(c, TILE)] = mm(norm[...], wq[:, pl.ds(c, TILE)]).astype(BF)

    tiles(local, TILE, query)

    ids = [span[j] for j in range(total)]
    run = [jnp.int32(0)] * spans
    inv = []
    for j in range(total):
        at = jnp.int32(-1)
        for c in range(spans):
            hit = (ids[j] == c).astype(jnp.int32)
            at = at + hit * (c * KMAX + 1 + run[c])
            run[c] = run[c] + hit
        inv.append(at)
    for i in range(spans * KMAX):
        at = jnp.int32(0)
        for j in range(1, total):
            at = at + (inv[j] == i).astype(jnp.int32) * j
        big[i] = kv[at]
    wave(n_seq + 1)
    arrived("o")

    def z_sends():
        found = []
        for k in range(1, n_seq):
            peer = lax.rem(s + k, n_seq)
            found.append(remote(cols(dout, peer, piece), rows_of(dcol, s, tokens), ks.at[0, k], kr.at[0, k], {"seq": peer}))
        return found

    dcol_sends = z_sends()
    for c in dcol_sends:
        c.start()
    dcol[pl.ds(pl.multiple_of(s * tokens, tokens), tokens), :] = dout[:, pl.ds(pl.multiple_of(s * piece, 128), piece)]

    def d_context(c):
        da_s[:, pl.ds(c, TILE)] = dot(dout[...], wo[pl.ds(c, TILE), :], NT).astype(BF)

    tiles(local, TILE, d_context)

    keys = KMAX * NLEN
    factor = HD ** (-0.5)
    tok0 = pl.multiple_of(s * tokens, tokens)

    def head(h, _):
        hc = pl.ds(pl.multiple_of(h * HD, HD), HD)
        vc = pl.ds(pl.multiple_of(local + h * HD, HD), HD)
        for c in range(spans):
            tr, kr_, gr = pl.ds(c * CLEN, CLEN), pl.ds(c * KMAX, KMAX), pl.ds((spans + c) * KMAX, KMAX)
            q, da = q_s[tr, hc], da_s[tr, hc]
            k, v = big[kr_, :, hc].reshape(keys, HD), big[kr_, :, vc].reshape(keys, HD)
            scores = dot(q, k, NT) * factor
            spot = lax.broadcasted_iota(jnp.int32, scores.shape, 1)
            scores = jnp.where(spot < run[c] * NLEN, scores, -1e30)
            weights = jnp.exp(scores - jnp.max(scores, axis=-1, keepdims=True))
            probs = weights / jnp.sum(weights, axis=-1, keepdims=True)
            probs_b = probs.astype(BF)
            att[pl.ds(pl.multiple_of(tok0 + c * CLEN, CLEN), CLEN), hc] = mm(probs_b, v).astype(BF)
            d_probs = dot(da, v, NT)
            row_dot = jnp.sum(probs * d_probs, axis=-1, keepdims=True)
            d_scores = (probs * (d_probs - row_dot) * factor).astype(BF)
            dq_s[tr, hc] = mm(d_scores, k).astype(BF)
            big[gr, :, hc] = dot(d_scores, q, TN).astype(BF).reshape(KMAX, NLEN, HD)
            big[gr, :, vc] = dot(probs_b, da, TN).astype(BF).reshape(KMAX, NLEN, HD)
        return 0

    lax.fori_loop(0, heads, head, 0)

    att_own = rows_of(att, s, tokens)
    att_sends = [
        remote(att_own, att_own, ks.at[1, k], kr.at[1, k], {"seq": lax.rem(s + k, n_seq)}) for k in range(1, n_seq)
    ]
    for c in att_sends:
        c.start()

    for j in range(total):
        vals = big[spans * KMAX + jnp.clip(inv[j], 0, spans * KMAX - 1)]
        mark = jnp.full(vals.shape, inv[j], jnp.int32)
        kv[j] = jnp.where(mark >= 0, vals.astype(F32), 0.0).astype(BF)

    class Sum:
        def __init__(self, i, route, part, first, forward, last):
            self.i, self.part, self.r = i, part, (forward, first, last)
            self.near, self.far = (n ^ 1, n ^ 2) if route == 0 else (n ^ 2, n ^ 1)

        def copy(self, step):
            m = (n ^ 3, self.near, self.far)[step]
            dev = {"nbr": self.far if step == 2 else self.near}
            return remote(self.part(m), self.r[step], us.at[self.i, step], ur.at[self.i, step], dev)

        def second(self):
            self.copy(0).wait_recv()
            mine = self.part(self.far)
            mine[...] = (mine[...].astype(F32) + self.r[0][...].astype(F32)).astype(BF)
            self.copy(2).start()

        def result(self):
            self.copy(1).wait_recv()
            self.copy(2).wait_recv()
            return self.part(n)[...].astype(F32) + self.r[1][...].astype(F32) + self.r[2][...].astype(F32)

    enc_sums = [
        Sum(j, 0 if j < half_slots else 1, lambda m, j=j: big.at[m * slots + j, :, pl.ds(0, width)], e1.at[j], e2.at[j], e3.at[j])
        for j in range(slots)
    ]
    hr = tokens // 2
    out_sums = [
        Sum(slots + h, h, lambda m, h=h: po.at[m, pl.ds(h * hr, hr)], ro.at[0, h], ro.at[1, h], ro.at[2, h])
        for h in (0, 1)
    ]
    dn_sums = [
        Sum(slots + 2 + h, h, lambda m, h=h: pd.at[m, pl.ds(h * hr, hr)], rd.at[0, h], rd.at[1, h], rd.at[2, h])
        for h in (0, 1)
    ]

    def back(m, j):
        slot = pl.ds(m * slots + j, half_slots)
        vals = kv[slot].reshape(unit, 2 * local)
        for c in range(0, width, TILE):
            w = min(TILE, width - c)
            big[slot, :, c : c + w] = dot(vals, wkv[c : c + w, :], NT).astype(BF).reshape(half_slots, NLEN, w)

    sets = (range(0, half_slots), range(half_slots, slots))
    for h in (0, 1):
        back(n ^ 3, h * half_slots)
        for j in sets[h]:
            enc_sums[j].copy(0).start()

    def d_weights(c):
        pw[:, pl.ds(c, TILE)] = mm(enct[...], kv[:, :, pl.ds(c, TILE)].reshape(total * NLEN, TILE)).astype(BF)

    tiles(2 * local, TILE, d_weights)
    w_sends = []
    for k in range(1, n_seq):
        peer = lax.rem(s + k, n_seq)
        w_sends.append(remote(rows_of(pw, peer, wr_k), wr.at[k], ks.at[2, k], kr.at[2, k], {"seq": peer}))
    for c in w_sends:
        c.start()

    for h in (0, 1):
        back((n ^ 1, n ^ 2)[h], h * half_slots)
        for j in sets[h]:
            enc_sums[j].copy(1).start()

    def out_part(m):
        def tile(c):
            wc = pl.ds(pl.multiple_of(m * feat + c, TILE), TILE)
            po[m, :, pl.ds(c, TILE)] = mm(att[pl.ds(tok0, tokens), :], wo[:, wc]).astype(BF)

        tiles(feat, TILE, tile)

    def dn_part(m):
        def tile(c):
            wc = pl.ds(pl.multiple_of(m * feat + c, TILE), TILE)
            pd[m, :, pl.ds(c, TILE)] = dot(dq_s[...], wq[wc, :], NT).astype(BF)

        tiles(feat, TILE, tile)

    for make, group in ((out_part, out_sums), (dn_part, dn_sums)):
        make(n ^ 3)
        for u in group:
            u.copy(0).start()
        make(n ^ 1)
        make(n ^ 2)
        for u in group:
            u.copy(1).start()
        make(n)

    def stat_rows(r):
        acc = jnp.zeros((32, 1), F32)
        for m in range(n_nbr):
            vals = hid[pl.ds(r, 32), m * feat : (m + 1) * feat].astype(F32)
            grad = gains[m, 0:1].astype(F32) * pd[m, pl.ds(r, 32), :].astype(F32)
            acc = acc + jnp.sum(vals * grad, axis=-1, keepdims=True)
        rows = jnp.broadcast_to(acc / (n_nbr * feat), (32, HD))
        st[0, pl.ds(r, 32), :] = rows

    tiles(tokens, 32, stat_rows)
    st[4] = st[0].T
    stat_sends = [
        remote(st.at[4, pl.ds(0, 8)], st.at[1 + d, pl.ds(0, 8)], ss.at[4 + d], sr.at[4 + d], dev)
        for d, dev in enumerate((x, y, diag))
    ]
    for c in stat_sends:
        c.start()

    for h in (0, 1):
        back((n ^ 2, n ^ 1)[h], h * half_slots)
    for i in range(half_slots):
        enc_sums[i].second()
        enc_sums[half_slots + i].second()
    for h in (0, 1):
        back(n, h * half_slots)
    for u in out_sums + dn_sums:
        u.second()

    writes = []

    def write(src, dst):
        c = pltpu.make_async_copy(src, dst, osem.at[len(writes)])
        c.start()
        writes.append(c)

    for c in dcol_sends + att_sends:
        c.wait_recv()

    step = min(TILE, piece)

    def d_out_weights(c):
        dwo[:, pl.ds(c, step)] = dot(att[...], dcol[:, pl.ds(c, step)], TN)

    tiles(piece, step, d_out_weights)
    write(dwo, dwo_o)

    for c in w_sends:
        c.wait_recv()
    acc = rows_of(pw, s, wr_k)[...].astype(F32)
    for k in range(1, n_seq):
        acc = acc + wr[k].astype(F32)
    dwf[...] = acc
    write(dwf.at[:, pl.ds(0, local)], dwk_o)
    write(dwf.at[:, pl.ds(local, local)], dwv_o)

    for i in range(half_slots):
        for j in (i, half_slots + i):
            e1[j] = enc_sums[j].result().astype(BF)
            write(e1.at[j], denc_o.at[j])
    for h, u in enumerate(out_sums):
        vals = cols(hid, n, feat)[h * hr : (h + 1) * hr, :].astype(F32)
        ro[0, h] = (vals + u.result()).astype(BF)
        write(ro.at[0, h], out_o.at[pl.ds(h * hr, hr)])
    for c in stat_sends:
        c.wait_recv()
    stat_row = st[4, 0:1] + st[1, 0:1] + st[2, 0:1] + st[3, 0:1]
    stat = jnp.broadcast_to(stat_row, (tokens, tokens)).T
    for h, u in enumerate(dn_sums):
        rr = slice(h * hr, (h + 1) * hr)
        vals = cols(hid, n, feat)[rr, :].astype(F32)
        grad = gains[n, 0:1].astype(F32) * u.result()
        scale = rst[rr, 0:1]
        res = cols(dout, n, feat)[rr, :].astype(F32) + scale * grad - vals * scale**3 * stat[rr, 0:1]
        rd[0, h] = res.astype(BF)
        write(rd.at[0, h], dh_o.at[pl.ds(h * hr, hr)])

    @pl.when(has_right)
    def _():
        carry(right).wait_send()

    for a in order:
        for k in range(1, n_seq):
            for d in (0, 1):
                @pl.when(valid(d, k))
                def _(a=a, k=k, d=d):
                    share(a, k, d, b).wait_send()

                @pl.when(guard(d, k))
                def _(a=a, k=k, d=d):
                    ring(a, k, d).wait_send()
    for c in pair("h", 0) + pair("d", 1) + gain_sends + sums + stat_sends + dcol_sends + att_sends + w_sends:
        c.wait_send()
    for j in range(slots):
        for i in range(3):
            slot_copy(n, j, i, x).wait_send()
    for u in enc_sums + out_sums + dn_sums:
        for i in range(3):
            u.copy(i).wait_send()
    for c in writes:
        c.wait()


def layer(hidden, d_out, gain, emb, span, e_gain, w_cond, w_enc, w_q, w_k, w_v, w_o):
    n_seq, n_nbr = lax.axis_size("seq"), lax.axis_size("nbr")
    args = (hidden, d_out, gain, emb, span, e_gain, w_cond, w_enc, w_q, w_k, w_v, w_o)
    tokens, feat = hidden.shape
    slots, _, width = emb.shape
    total = slots * n_nbr
    local, piece, wr_k = w_q.shape[1], w_o.shape[1], w_k.shape[0]
    spans = tokens // CLEN
    full = feat * n_nbr
    vm = pltpu.VMEM
    dma = pltpu.SemaphoreType.DMA
    scratch = dict(
        hid=vm((tokens, full), BF), dout=vm((tokens, full), BF), gains=vm((n_nbr,) + gain.shape, BF),
        wq=vm((full, local), BF), wo=vm((local, full), BF), wkv=vm((width, 2 * local), BF),
        enc=vm((total * NLEN, width), BF), enct=vm((width, total * NLEN), BF),
        kv=vm((total, NLEN, 2 * local), BF), big=vm((2 * spans * KMAX, NLEN, 2 * local), BF),
        norm=vm((tokens, full), BF), rst=vm((tokens, HD), F32),
        e1=vm(emb.shape, BF), e2=vm(emb.shape, BF), e3=vm(emb.shape, BF),
        po=vm((n_nbr, tokens, feat), BF), pd=vm((n_nbr, tokens, feat), BF),
        ro=vm((3, 2, tokens // 2, feat), BF), rd=vm((3, 2, tokens // 2, feat), BF),
        q=vm((tokens, local), BF), da=vm((tokens, local), BF), dq=vm((tokens, local), BF),
        att=vm((n_seq * tokens, local), BF), dcol=vm((n_seq * tokens, piece), BF),
        pw=vm((width, 2 * local), BF), wr=vm((n_seq, wr_k, 2 * local), BF),
        dwo=vm((local, piece), F32), dwf=vm((wr_k, 2 * local), F32),
        emb=vm(emb.shape, BF), cond=vm(w_cond.shape, BF), wenc=vm(w_enc.shape, BF),
        pool=vm((2, 8, feat), F32), cpart=vm((8, width), F32), crecv=vm((3, 8, width), F32),
        st=vm((5, tokens, HD), F32),
        lsem=dma((10,)), osem=dma((slots + 8,)),
        zs=dma((4, n_seq, 2)), zr=dma((4, n_seq, 2)), ps=dma((4, n_seq, 2)), pr=dma((4, n_seq, 2)),
        ns=dma((3, 4)), nr=dma((3, 4)), es=dma((slots, 3)), er=dma((slots, 3)),
        ss=dma((7,)), sr=dma((7,)), us=dma((slots + 4, 3)), ur=dma((slots + 4, 3)),
        ks=dma((3, n_seq)), kr=dma((3, n_seq)),
    )
    specs = [ANY] * 12
    specs[4] = pl.BlockSpec(memory_space=pltpu.SMEM)
    specs[5] = pl.BlockSpec(memory_space=pltpu.VMEM)
    shapes = [
        jax.ShapeDtypeStruct(hidden.shape, BF), jax.ShapeDtypeStruct(hidden.shape, BF),
        jax.ShapeDtypeStruct(emb.shape, BF), jax.ShapeDtypeStruct(w_o.shape, F32),
        jax.ShapeDtypeStruct(w_k.shape, F32), jax.ShapeDtypeStruct(w_v.shape, F32),
    ]
    return pl.pallas_call(
        functools.partial(layer_kernel, n_seq, n_nbr, tuple(scratch)),
        out_shape=shapes,
        in_specs=specs,
        out_specs=[ANY] * 6,
        scratch_shapes=list(scratch.values()),
        compiler_params=pltpu.CompilerParams(
            collective_id=0, has_side_effects=True, vmem_limit_bytes=67043328
        ),
        name="layer",
    )(*args)


def body(hidden, d_out, nbr_emb, slot_span, dec_gain, enc_gain, w_cond, w_enc, w_q, w_k, w_v, w_o):
    gain = jnp.broadcast_to(dec_gain[None], (16, dec_gain.shape[0]))
    return tuple(layer(
        hidden, d_out, gain, nbr_emb, slot_span, enc_gain[None], w_cond, w_enc, w_q, w_k, w_v, w_o
    ))


def solution(mesh):
    placed = (
        P(("batch", "seq"), "nbr"),
        P(("batch", "seq"), "nbr"),
        P(("batch", "seq", "nbr"), None, None),
        P(("batch", "seq")),
        P("nbr"),
        P(),
        P("nbr", None),
        P(),
        P("seq", "nbr"),
        P("seq", "nbr"),
        P("seq", "nbr"),
        P("nbr", "seq"),
    )
    return jax.shard_map(
        body,
        mesh=mesh,
        in_specs=placed,
        out_specs=(
            P(("batch", "seq"), "nbr"),
            P(("batch", "seq"), "nbr"),
            P(("batch", "seq", "nbr"), None, None),
            P(("batch", "nbr"), "seq"),
            P(("batch", "seq"), "nbr"),
            P(("batch", "seq"), "nbr"),
        ),
        check_vma=False,
    )
```

```python
import functools

import jax
import jax.numpy as jnp
from jax import lax
from jax.experimental import pallas as pl
from jax.experimental.pallas import tpu as pltpu
from jax.sharding import PartitionSpec as P

HD = 128
CLEN = 64
NLEN = 128
KMAX = 8
BF = jnp.bfloat16
F32 = jnp.float32
MESH = pl.DeviceIdType.MESH
ANY = pl.BlockSpec(memory_space=pl.ANY)
NT = (((1,), (1,)), ((), ()))
TN = (((0,), (0,)), ((), ()))
TILE = 256

dot = functools.partial(lax.dot_general, preferred_element_type=F32)


def mm(a, b):
    return jnp.dot(a, b, preferred_element_type=F32)


def remote(src, dst, send, recv, dev):
    return pltpu.make_async_remote_copy(
        src_ref=src, dst_ref=dst, send_sem=send, recv_sem=recv, device_id=dev, device_id_type=MESH
    )


def cols(ref, i, width):
    return ref.at[:, pl.ds(pl.multiple_of(i * width, 128), width)]


def rows_of(ref, i, count):
    return ref.at[pl.ds(pl.multiple_of(i * count, 8), count)]


def tiles(count, step, body):
    def one(t, _):
        body(pl.multiple_of(t * step, step))
        return 0

    lax.fori_loop(0, count // step, one, 0)


def layer_kernel(n_seq, n_nbr, names, *refs):
    hidden, d_out, gain, emb, span, w_cond, w_enc, w_q, w_k, w_v, w_o = refs[:11]
    out_o, dh_o, denc_o, dwo_o, dwk_o, dwv_o = refs[11:17]
    S = dict(zip(names, refs[17:]))
    hid, dout, gains, wq, wo, wkv = (S[k] for k in ("hid", "dout", "gains", "wq", "wo", "wkv"))
    enc, enct, kv, big, norm, rst = (S[k] for k in ("enc", "enct", "kv", "big", "norm", "rst"))
    prob = S["prob"]
    e1, e2, e3, po, pd = (S[k] for k in ("e1", "e2", "e3", "po", "pd"))
    ro, rd, q_s, da_s, dq_s = (S[k] for k in ("ro", "rd", "q", "da", "dq"))
    att, dcol, pw, wr, dwo, dwf = (S[k] for k in ("att", "dcol", "pw", "wr", "dwo", "dwf"))
    emb_v, cond_v, enc_v, pool = (S[k] for k in ("emb", "cond", "wenc", "pool"))
    cpart, crecv, st = (S[k] for k in ("cpart", "crecv", "st"))
    lsem, osem, zs, zr, ps, pr = (S[k] for k in ("lsem", "osem", "zs", "zr", "ps", "pr"))
    ns, nr, es, er, ss, sr = (S[k] for k in ("ns", "nr", "es", "er", "ss", "sr"))
    us, ur, ks, kr = (S[k] for k in ("us", "ur", "ks", "kr"))

    s, n, b = lax.axis_index("seq"), lax.axis_index("nbr"), lax.axis_index("batch")
    x, y, core, diag = {"nbr": n ^ 1}, {"nbr": n ^ 2}, {"batch": 1 - b}, {"nbr": n ^ 3}
    right, left = {"seq": s + 1}, {"seq": s - 1}
    has_right, has_left = s + 1 < n_seq, s > 0
    tokens, feat = hidden.shape
    spans = tokens // CLEN
    slots, width = emb.shape[0], emb.shape[2]
    total = slots * n_nbr
    local = w_q.shape[1]
    heads = local // HD
    half_slots = slots // 2
    unit = half_slots * NLEN
    wr_q, wr_k, piece = w_q.shape[0], w_k.shape[0], w_o.shape[1]

    own = {
        "h": cols(hid, n, feat), "d": cols(dout, n, feat), "g": gains.at[n],
        "k": rows_of(wkv, s, wr_k).at[:, pl.ds(0, local)],
        "v": rows_of(wkv, s, wr_k).at[:, pl.ds(local, local)],
        "q": rows_of(wq, s, wr_q), "o": cols(wo, s, piece),
    }
    source = {"h": hidden, "d": d_out, "g": gain.at[:, pl.ds(0, feat)], "k": w_k, "v": w_v, "q": w_q, "o": w_o}
    loads = {
        k: pltpu.make_async_copy(source[k], own[k], lsem.at[i]) for i, k in enumerate(("h", "d", "g", "k", "v", "q", "o"))
    }
    loads["c"] = pltpu.make_async_copy(w_cond, cond_v, lsem.at[7])
    loads["e"] = pltpu.make_async_copy(emb, emb_v, lsem.at[8])
    loads["w"] = pltpu.make_async_copy(w_enc, enc_v, lsem.at[9])
    loads["n"] = pltpu.make_async_copy(gain.at[:, pl.ds(feat, width)], S["egain"], lsem.at[10])
    for k in ("h", "k", "v", "q", "g", "c", "d", "e", "w", "n", "o"):
        loads[k].start()

    barrier = pltpu.get_barrier_semaphore()
    for dev in (x, y, diag, core):
        pl.semaphore_signal(barrier, inc=1, device_id=dev, device_id_type=MESH)
    for k in range(1, n_seq):
        pl.semaphore_signal(barrier, inc=1, device_id={"seq": lax.rem(s + k, n_seq)}, device_id_type=MESH)

    loads["h"].wait()
    means = []
    for c in range(spans):
        part = cols(hid, n, feat)[c * CLEN : (c + 1) * CLEN, :].astype(F32)
        means.append((jnp.sum(part, axis=0, keepdims=True) / CLEN).astype(BF).astype(F32))
    pool[0] = jnp.broadcast_to(means[spans - 1], pool.shape[1:])
    pl.semaphore_wait(barrier, n_seq + 3)

    def carry(dev):
        return remote(pool.at[0], pool.at[1], ss.at[0], sr.at[0], dev)

    @pl.when(has_right)
    def _():
        carry(right).start()

    order = ("k", "v", "q", "o")

    def block(a, j):
        if a == "k":
            return rows_of(wkv, j, wr_k).at[:, pl.ds(0, local)]
        if a == "v":
            return rows_of(wkv, j, wr_k).at[:, pl.ds(local, local)]
        if a == "q":
            return rows_of(wq, j, wr_q)
        return cols(wo, j, piece)

    def half(a, j, h):
        if a in ("k", "v"):
            w = local // 2
            base = 0 if a == "k" else local
            return rows_of(wkv, j, wr_k).at[:, pl.ds(pl.multiple_of(base + h * w, 128), w)]
        if a == "q":
            c = wr_q // 2
            return wq.at[pl.ds(pl.multiple_of(j * wr_q + h * c, 8), c)]
        c = local // 2
        return wo.at[pl.ds(pl.multiple_of(h * c, 8), c), pl.ds(pl.multiple_of(j * piece, 128), piece)]

    def ring(a, k, d):
        j = s - k + 1 if d == 0 else s + k - 1
        i = order.index(a)
        part = half(a, j, b)
        return remote(part, part, zs.at[i, k, d], zr.at[i, k, d], right if d == 0 else left)

    def guard(d, k):
        if d == 0:
            return has_right & (s - (k - 1) >= 0)
        return has_left & (s + (k - 1) < n_seq)

    def valid(d, k):
        return (s - k >= 0) if d == 0 else (s + k < n_seq)

    def launch(a):
        loads[a].wait()
        for d in (0, 1):
            @pl.when(guard(d, 1))
            def _(a=a, d=d):
                ring(a, 1, d).start()

    def share(a, k, d, h):
        j = s - k if d == 0 else s + k
        i = order.index(a)
        part = half(a, j, h)
        return remote(part, part, ps.at[i, k, d], pr.at[i, k, d], core)

    def relay(a, k, kind="all"):
        i = order.index(a)
        for d in (0, 1):
            onward = guard(d, k + 1) if k + 1 < n_seq else valid(d, k) & (s < 0)
            when = {"all": valid(d, k), "on": onward, "end": valid(d, k) & jnp.logical_not(onward)}[kind]

            @pl.when(when)
            def _(d=d):
                part = half(a, s - k if d == 0 else s + k, b)
                remote(part, part, zs.at[i, k, d], zr.at[i, k, d], left if d == 0 else right).wait_recv()
                share(a, k, d, b).start()

            if k + 1 < n_seq and kind != "end":
                @pl.when(guard(d, k + 1))
                def _(d=d):
                    ring(a, k + 1, d).start()

    def arrived(a):
        for k in range(1, n_seq):
            for d in (0, 1):
                @pl.when(valid(d, k))
                def _(k=k, d=d):
                    share(a, k, d, 1 - b).wait_recv()

    def wave(w, skip=()):
        for a, lag in (("k", 0), ("v", 0), ("q", 1), ("o", 2)):
            if 1 <= w - lag < n_seq and a not in skip:
                relay(a, w - lag, "on" if a == "o" else "all")

    for a in ("k", "v", "q"):
        launch(a)

    def pair(key, i):
        ref = own[key]
        return [remote(ref, ref, ns.at[i, d], nr.at[i, d], dev) for d, dev in enumerate((x, y))]

    for c in pair("h", 0):
        c.start()
    loads["g"].wait()
    gain_sends = [
        remote(own["g"], own["g"], ns.at[2, d], nr.at[2, d], dev) for d, dev in enumerate((x, y, diag))
    ]
    for c in gain_sends:
        c.start()

    @pl.when(has_left)
    def _():
        carry(left).wait_recv()

    @pl.when(jnp.logical_not(has_left))
    def _():
        pool[1] = jnp.zeros(pool.shape[1:], F32)

    place = lax.broadcasted_iota(jnp.int32, pool.shape[1:], 0)
    before = pool[1]
    for c in range(1, spans):
        before = jnp.where(place == c, jnp.broadcast_to(means[c - 1], before.shape), before)
    loads["c"].wait()
    cpart[...] = mm(before.astype(BF), cond_v[...])
    sums = [remote(cpart, crecv.at[d], ss.at[1 + d], sr.at[1 + d], dev) for d, dev in enumerate((x, y, diag))]
    for c in sums:
        c.start()
    loads["d"].wait()
    for c in pair("d", 1):
        c.start()
    for c in sums:
        c.wait_recv()
    condition = cpart[...] + crecv[0] + crecv[1] + crecv[2]

    def slot_rows(m, j):
        return pl.ds(pl.multiple_of((m * slots + j) * NLEN, NLEN), NLEN)

    def slot_copy(src, j, i, dev):
        part = enc.at[slot_rows(src, j)]
        return remote(part, part, es.at[j, i], er.at[j, i], dev)

    loads["e"].wait()
    loads["w"].wait()
    loads["n"].wait()
    gain_row = S["egain"][0:1].astype(F32)
    for j in range(slots):
        mark = jnp.full((1, width), span[n * slots + j], jnp.int32)
        vals = emb_v[j].astype(F32)
        for c in range(spans):
            vals = vals + jnp.where(mark == c, condition[c : c + 1], 0.0)
        scale = lax.rsqrt(jnp.mean(vals * vals, axis=-1, keepdims=True) + 1e-06)
        mixed = mm((vals * scale * gain_row).astype(BF), enc_v[...])
        enc[slot_rows(n, j), :] = (vals + mixed / (1.0 + jnp.exp(-mixed))).astype(BF)
        slot_copy(n, j, 0, x).start()
        slot_copy(n, j, 1, y).start()
        if j == half_slots:
            wave(1)
            launch("o")

    def diagonal(ref, i):
        c = tokens // 2
        for d, (src, dev) in enumerate(((n ^ 1, y), (n ^ 2, x))):
            full = cols(ref, src, feat)
            remote(full, full, ns.at[i, d], nr.at[i, d], dev).wait_recv()
            part = full.at[pl.ds(d * c, c)]
            remote(part, part, ns.at[i, 2 + d], nr.at[i, 2 + d], dev).start()

    def diagonal_done(ref, i):
        c = tokens // 2
        for d in (0, 1):
            part = cols(ref, n ^ 3, feat).at[pl.ds(d * c, c)]
            remote(part, part, ns.at[i, 2 + d], nr.at[i, 2 + d], x).wait()

    def pass_on(j):
        for d, (src, dev) in enumerate(((n ^ 1, y), (n ^ 2, x))):
            slot_copy(src, j, d, dev).wait_recv()
            if j % 2 == d:
                slot_copy(src, j, 2, dev).start()

    def project(m, j):
        at = pl.multiple_of((m * slots + j) * NLEN, NLEN)
        slot = pl.ds(m * slots + j, half_slots)
        block_rows = enc[pl.ds(at, unit), :]
        enct[:, pl.ds(at, unit)] = block_rows.T

        def tile(c):
            res = mm(enc[pl.ds(at, unit), :], wkv[:, pl.ds(c, TILE)]).astype(BF)
            kv[slot, :, pl.ds(c, TILE)] = res.reshape(half_slots, NLEN, TILE)

        tiles(2 * local, TILE, tile)

    diagonal(hid, 0)
    diagonal(dout, 1)
    wave(2)
    for j in range(half_slots):
        pass_on(j)
    diagonal_done(hid, 0)
    diagonal_done(dout, 1)
    for c in gain_sends:
        c.wait_recv()

    def norm_rows(r):
        part = hid[pl.ds(r, 32), :].astype(F32)
        scale = lax.rsqrt(jnp.mean(part * part, axis=-1, keepdims=True) + 1e-06)
        rst[pl.ds(r, 32), :] = jnp.broadcast_to(scale, (32, HD))
        for m in range(n_nbr):
            vals = hid[pl.ds(r, 32), m * feat : (m + 1) * feat].astype(F32) * scale * gains[m, 0:1].astype(F32)
            norm[pl.ds(r, 32), m * feat : (m + 1) * feat] = vals.astype(BF)

    tiles(tokens, 32, norm_rows)
    wave(3)
    for w in range(4, n_seq):
        wave(w)
    for j in range(half_slots, slots):
        pass_on(j)
    arrived("k")
    arrived("v")
    for m in (n, n ^ 1, n ^ 2):
        project(m, 0)
    wave(n_seq)
    for m in (n, n ^ 1, n ^ 2):
        project(m, half_slots)
    for j in range(slots):
        slot_copy(n ^ 3, j, 2, x).wait_recv()
        if (j + 1) % half_slots == 0:
            project(n ^ 3, j + 1 - half_slots)
    arrived("q")

    def query(c):
        q_s[:, pl.ds(c, TILE)] = mm(norm[...], wq[:, pl.ds(c, TILE)]).astype(BF)

    tiles(local, TILE, query)

    ids = [span[j] for j in range(total)]
    run = [jnp.int32(0)] * spans
    inv = []
    for j in range(total):
        at = jnp.int32(-1)
        for c in range(spans):
            hit = (ids[j] == c).astype(jnp.int32)
            at = at + hit * (c * KMAX + 1 + run[c])
            run[c] = run[c] + hit
        inv.append(at)
    for i in range(spans * KMAX):
        at = jnp.int32(0)
        for j in range(1, total):
            at = at + (inv[j] == i).astype(jnp.int32) * j
        big[i] = kv[at]

    keys = KMAX * NLEN
    factor = HD ** (-0.5)
    tok0 = pl.multiple_of(s * tokens, tokens)

    spot = lax.broadcasted_iota(jnp.int32, (1, keys), 1)
    bias = [jnp.where(spot < run[c] * NLEN, 0.0, -1e30) for c in range(spans)]

    def forward(h, _):
        hc = pl.ds(pl.multiple_of(h * HD, HD), HD)
        vc = pl.ds(pl.multiple_of(local + h * HD, HD), HD)
        for c in range(spans):
            kc = pl.ds(c * KMAX, KMAX)
            k, v = big[kc, :, hc].reshape(keys, HD), big[kc, :, vc].reshape(keys, HD)
            scores = dot(q_s[pl.ds(c * CLEN, CLEN), hc], k, NT) * factor + bias[c]
            weights = jnp.exp(scores - jnp.max(scores, axis=-1, keepdims=True))
            probs = weights * (1.0 / jnp.sum(weights, axis=-1, keepdims=True))
            prob[c, h] = probs
            att[pl.ds(pl.multiple_of(tok0 + c * CLEN, CLEN), CLEN), hc] = mm(probs.astype(BF), v).astype(BF)
        return 0

    lax.fori_loop(0, heads, forward, 0)
    for k in range(1, n_seq):
        relay("o", k, "end")
    arrived("o")

    def d_context(c):
        da_s[:, pl.ds(c, TILE)] = dot(dout[...], wo[pl.ds(c, TILE), :], NT).astype(BF)

    tiles(local, TILE, d_context)

    def backward(h, _):
        hc = pl.ds(pl.multiple_of(h * HD, HD), HD)
        vc = pl.ds(pl.multiple_of(local + h * HD, HD), HD)
        for c in range(spans):
            tr, kc, gc = pl.ds(c * CLEN, CLEN), pl.ds(c * KMAX, KMAX), pl.ds((spans + c) * KMAX, KMAX)
            q, da, probs = q_s[tr, hc], da_s[tr, hc], prob[c, h]
            k, v = big[kc, :, hc].reshape(keys, HD), big[kc, :, vc].reshape(keys, HD)
            d_probs = dot(da, v, NT)
            row_dot = jnp.sum(probs * d_probs, axis=-1, keepdims=True)
            d_scores = (probs * (d_probs - row_dot) * factor).astype(BF)
            dq_s[tr, hc] = mm(d_scores, k).astype(BF)
            big[gc, :, hc] = dot(d_scores, q, TN).astype(BF).reshape(KMAX, NLEN, HD)
            big[gc, :, vc] = dot(probs.astype(BF), da, TN).astype(BF).reshape(KMAX, NLEN, HD)
        return 0

    lax.fori_loop(0, heads, backward, 0)

    att_own = rows_of(att, s, tokens)
    att_sends = [
        remote(att_own, att_own, ks.at[1, k], kr.at[1, k], {"seq": lax.rem(s + k, n_seq)}) for k in range(1, n_seq)
    ]
    for c in att_sends:
        c.start()

    for j in range(total):
        vals = big[spans * KMAX + jnp.clip(inv[j], 0, spans * KMAX - 1)]
        mark = jnp.full(vals.shape, inv[j], jnp.int32)
        kv[j] = jnp.where(mark >= 0, vals.astype(F32), 0.0).astype(BF)

    class Sum:
        def __init__(self, i, route, part, first, forward, last):
            self.i, self.part, self.r = i, part, (forward, first, last)
            self.near, self.far = (n ^ 1, n ^ 2) if route == 0 else (n ^ 2, n ^ 1)

        def copy(self, step):
            m = (n ^ 3, self.near, self.far)[step]
            dev = {"nbr": self.far if step == 2 else self.near}
            return remote(self.part(m), self.r[step], us.at[self.i, step], ur.at[self.i, step], dev)

        def second(self):
            self.copy(0).wait_recv()
            mine = self.part(self.far)
            mine[...] = (mine[...].astype(F32) + self.r[0][...].astype(F32)).astype(BF)
            self.copy(2).start()

        def result(self):
            self.copy(1).wait_recv()
            self.copy(2).wait_recv()
            return self.part(n)[...].astype(F32) + self.r[1][...].astype(F32) + self.r[2][...].astype(F32)

    enc_sums = [
        Sum(j, 0 if j < half_slots else 1, lambda m, j=j: big.at[m * slots + j, :, pl.ds(0, width)], e1.at[j], e2.at[j], e3.at[j])
        for j in range(slots)
    ]
    hr = tokens // 2
    out_sums = [
        Sum(slots + h, h, lambda m, h=h: po.at[m, pl.ds(h * hr, hr)], ro.at[0, h], ro.at[1, h], ro.at[2, h])
        for h in (0, 1)
    ]
    dn_sums = [
        Sum(slots + 2 + h, h, lambda m, h=h: pd.at[m, pl.ds(h * hr, hr)], rd.at[0, h], rd.at[1, h], rd.at[2, h])
        for h in (0, 1)
    ]

    def back(m, j):
        slot = pl.ds(m * slots + j, half_slots)
        vals = kv[slot].reshape(unit, 2 * local)
        for c in range(0, width, TILE):
            w = min(TILE, width - c)
            big[slot, :, c : c + w] = dot(vals, wkv[c : c + w, :], NT).astype(BF).reshape(half_slots, NLEN, w)

    sets = (range(0, half_slots), range(half_slots, slots))
    for h in (0, 1):
        back(n ^ 3, h * half_slots)
        for j in sets[h]:
            enc_sums[j].copy(0).start()

    def d_weights(c):
        pw[:, pl.ds(c, TILE)] = mm(enct[...], kv[:, :, pl.ds(c, TILE)].reshape(total * NLEN, TILE)).astype(BF)

    tiles(2 * local, TILE, d_weights)
    w_sends = []
    for k in range(1, n_seq):
        peer = lax.rem(s + k, n_seq)
        w_sends.append(remote(rows_of(pw, peer, wr_k), wr.at[k], ks.at[2, k], kr.at[2, k], {"seq": peer}))
    for c in w_sends:
        c.start()

    def z_sends():
        found = []
        for k in range(1, n_seq):
            peer = lax.rem(s + k, n_seq)
            found.append(remote(cols(dout, peer, piece), rows_of(dcol, s, tokens), ks.at[0, k], kr.at[0, k], {"seq": peer}))
        return found

    dcol_sends = z_sends()
    for c in dcol_sends:
        c.start()
    dcol[pl.ds(pl.multiple_of(s * tokens, tokens), tokens), :] = dout[:, pl.ds(pl.multiple_of(s * piece, 128), piece)]


    for h in (0, 1):
        back((n ^ 1, n ^ 2)[h], h * half_slots)
        for j in sets[h]:
            enc_sums[j].copy(1).start()

    def out_part(m):
        def tile(c):
            wc = pl.ds(pl.multiple_of(m * feat + c, TILE), TILE)
            po[m, :, pl.ds(c, TILE)] = mm(att[pl.ds(tok0, tokens), :], wo[:, wc]).astype(BF)

        tiles(feat, TILE, tile)

    def dn_part(m):
        def tile(c):
            wc = pl.ds(pl.multiple_of(m * feat + c, TILE), TILE)
            pd[m, :, pl.ds(c, TILE)] = dot(dq_s[...], wq[wc, :], NT).astype(BF)

        tiles(feat, TILE, tile)

    for make, group in ((out_part, out_sums), (dn_part, dn_sums)):
        make(n ^ 3)
        for u in group:
            u.copy(0).start()
        make(n ^ 1)
        make(n ^ 2)
        for u in group:
            u.copy(1).start()
        make(n)

    def stat_rows(r):
        acc = jnp.zeros((32, 1), F32)
        for m in range(n_nbr):
            vals = hid[pl.ds(r, 32), m * feat : (m + 1) * feat].astype(F32)
            grad = gains[m, 0:1].astype(F32) * pd[m, pl.ds(r, 32), :].astype(F32)
            acc = acc + jnp.sum(vals * grad, axis=-1, keepdims=True)
        rows = jnp.broadcast_to(acc / (n_nbr * feat), (32, HD))
        st[0, pl.ds(r, 32), :] = rows

    tiles(tokens, 32, stat_rows)
    st[4] = st[0].T
    stat_sends = [
        remote(st.at[4, pl.ds(0, 8)], st.at[1 + d, pl.ds(0, 8)], ss.at[4 + d], sr.at[4 + d], dev)
        for d, dev in enumerate((x, y, diag))
    ]
    for c in stat_sends:
        c.start()

    for h in (0, 1):
        back((n ^ 2, n ^ 1)[h], h * half_slots)
    for i in range(half_slots):
        enc_sums[i].second()
        enc_sums[half_slots + i].second()
    for h in (0, 1):
        back(n, h * half_slots)
    for u in out_sums + dn_sums:
        u.second()

    writes = []

    def write(src, dst):
        c = pltpu.make_async_copy(src, dst, osem.at[len(writes)])
        c.start()
        writes.append(c)

    for c in dcol_sends + att_sends:
        c.wait_recv()

    step = min(TILE, piece)

    def d_out_weights(c):
        dwo[:, pl.ds(c, step)] = dot(att[...], dcol[:, pl.ds(c, step)], TN)

    tiles(piece, step, d_out_weights)
    write(dwo, dwo_o)

    for c in w_sends:
        c.wait_recv()
    acc = rows_of(pw, s, wr_k)[...].astype(F32)
    for k in range(1, n_seq):
        acc = acc + wr[k].astype(F32)
    dwf[...] = acc
    write(dwf.at[:, pl.ds(0, local)], dwk_o)
    write(dwf.at[:, pl.ds(local, local)], dwv_o)

    for i in range(half_slots):
        for j in (i, half_slots + i):
            e1[j] = enc_sums[j].result().astype(BF)
            write(e1.at[j], denc_o.at[j])
    for h, u in enumerate(out_sums):
        vals = cols(hid, n, feat)[h * hr : (h + 1) * hr, :].astype(F32)
        ro[0, h] = (vals + u.result()).astype(BF)
        write(ro.at[0, h], out_o.at[pl.ds(h * hr, hr)])
    for c in stat_sends:
        c.wait_recv()
    stat_row = st[4, 0:1] + st[1, 0:1] + st[2, 0:1] + st[3, 0:1]
    stat = jnp.broadcast_to(stat_row, (tokens, tokens)).T
    for h, u in enumerate(dn_sums):
        rr = slice(h * hr, (h + 1) * hr)
        vals = cols(hid, n, feat)[rr, :].astype(F32)
        grad = gains[n, 0:1].astype(F32) * u.result()
        scale = rst[rr, 0:1]
        res = cols(dout, n, feat)[rr, :].astype(F32) + scale * grad - vals * scale**3 * stat[rr, 0:1]
        rd[0, h] = res.astype(BF)
        write(rd.at[0, h], dh_o.at[pl.ds(h * hr, hr)])

    @pl.when(has_right)
    def _():
        carry(right).wait_send()

    for a in order:
        for k in range(1, n_seq):
            for d in (0, 1):
                @pl.when(valid(d, k))
                def _(a=a, k=k, d=d):
                    share(a, k, d, b).wait_send()

                @pl.when(guard(d, k))
                def _(a=a, k=k, d=d):
                    ring(a, k, d).wait_send()
    for c in pair("h", 0) + pair("d", 1) + gain_sends + sums + stat_sends + dcol_sends + att_sends + w_sends:
        c.wait_send()
    for j in range(slots):
        for i in range(3):
            slot_copy(n, j, i, x).wait_send()
    for u in enc_sums + out_sums + dn_sums:
        for i in range(3):
            u.copy(i).wait_send()
    for c in writes:
        c.wait()


def layer(hidden, d_out, gain, emb, span, w_cond, w_enc, w_q, w_k, w_v, w_o):
    n_seq, n_nbr = lax.axis_size("seq"), lax.axis_size("nbr")
    args = (hidden, d_out, gain, emb, span, w_cond, w_enc, w_q, w_k, w_v, w_o)
    tokens, feat = hidden.shape
    slots, _, width = emb.shape
    total = slots * n_nbr
    local, piece, wr_k = w_q.shape[1], w_o.shape[1], w_k.shape[0]
    spans = tokens // CLEN
    full = feat * n_nbr
    vm = pltpu.VMEM
    dma = pltpu.SemaphoreType.DMA
    scratch = dict(
        hid=vm((tokens, full), BF), dout=vm((tokens, full), BF), gains=vm((n_nbr, gain.shape[0], feat), BF), egain=vm((gain.shape[0], width), BF),
        wq=vm((full, local), BF), wo=vm((local, full), BF), wkv=vm((width, 2 * local), BF),
        enc=vm((total * NLEN, width), BF), enct=vm((width, total * NLEN), BF),
        kv=vm((total, NLEN, 2 * local), BF), big=vm((2 * spans * KMAX, NLEN, 2 * local), BF),
        norm=vm((tokens, full), BF), prob=vm((spans, local // HD, CLEN, KMAX * NLEN), F32), rst=vm((tokens, HD), F32),
        e1=vm(emb.shape, BF), e2=vm(emb.shape, BF), e3=vm(emb.shape, BF),
        po=vm((n_nbr, tokens, feat), BF), pd=vm((n_nbr, tokens, feat), BF),
        ro=vm((3, 2, tokens // 2, feat), BF), rd=vm((3, 2, tokens // 2, feat), BF),
        q=vm((tokens, local), BF), da=vm((tokens, local), BF), dq=vm((tokens, local), BF),
        att=vm((n_seq * tokens, local), BF), dcol=vm((n_seq * tokens, piece), BF),
        pw=vm((width, 2 * local), BF), wr=vm((n_seq, wr_k, 2 * local), BF),
        dwo=vm((local, piece), F32), dwf=vm((wr_k, 2 * local), F32),
        emb=vm(emb.shape, BF), cond=vm(w_cond.shape, BF), wenc=vm(w_enc.shape, BF),
        pool=vm((2, 8, feat), F32), cpart=vm((8, width), F32), crecv=vm((3, 8, width), F32),
        st=vm((5, tokens, HD), F32),
        lsem=dma((11,)), osem=dma((slots + 8,)),
        zs=dma((4, n_seq, 2)), zr=dma((4, n_seq, 2)), ps=dma((4, n_seq, 2)), pr=dma((4, n_seq, 2)),
        ns=dma((3, 4)), nr=dma((3, 4)), es=dma((slots, 3)), er=dma((slots, 3)),
        ss=dma((7,)), sr=dma((7,)), us=dma((slots + 4, 3)), ur=dma((slots + 4, 3)),
        ks=dma((3, n_seq)), kr=dma((3, n_seq)),
    )
    specs = [ANY] * 11
    specs[4] = pl.BlockSpec(memory_space=pltpu.SMEM)
    shapes = [
        jax.ShapeDtypeStruct(hidden.shape, BF), jax.ShapeDtypeStruct(hidden.shape, BF),
        jax.ShapeDtypeStruct(emb.shape, BF), jax.ShapeDtypeStruct(w_o.shape, F32),
        jax.ShapeDtypeStruct(w_k.shape, F32), jax.ShapeDtypeStruct(w_v.shape, F32),
    ]
    return pl.pallas_call(
        functools.partial(layer_kernel, n_seq, n_nbr, tuple(scratch)),
        out_shape=shapes,
        in_specs=specs,
        out_specs=[ANY] * 6,
        scratch_shapes=list(scratch.values()),
        compiler_params=pltpu.CompilerParams(
            collective_id=0, has_side_effects=True, vmem_limit_bytes=67043328
        ),
        name="layer",
    )(*args)


def settle_kernel(*refs):
    count = len(refs) // 3
    ins, outs, bufs = refs[:count], refs[count : 2 * count], refs[2 * count : 3 * count]
    sems = refs[3 * count]
    loads = [pltpu.make_async_copy(a, v, sems.at[0, i]) for i, (a, v) in enumerate(zip(ins, bufs))]
    stores = [pltpu.make_async_copy(v, o, sems.at[1, i]) for i, (v, o) in enumerate(zip(bufs, outs))]
    for c in loads:
        c.start()
    for a, c in zip(loads, stores):
        a.wait()
        c.start()
    for c in stores:
        c.wait()


def settle(*arrays):
    count = len(arrays)
    return pl.pallas_call(
        settle_kernel,
        out_shape=[jax.ShapeDtypeStruct(v.shape, v.dtype) for v in arrays],
        in_specs=[ANY] * count,
        out_specs=[ANY] * count,
        scratch_shapes=[pltpu.VMEM(v.shape, v.dtype) for v in arrays] + [pltpu.SemaphoreType.DMA((2, count))],
        compiler_params=pltpu.CompilerParams(vmem_limit_bytes=60 * 2**20),
        name="settle",
    )(*arrays)


def body(hidden, d_out, nbr_emb, slot_span, dec_gain, enc_gain, w_cond, w_enc, w_q, w_k, w_v, w_o):
    both = jnp.concatenate([dec_gain, enc_gain])
    gain = jnp.broadcast_to(both[None], (16, both.shape[0]))
    return tuple(settle(*layer(
        hidden, d_out, gain, nbr_emb, slot_span, w_cond, w_enc, w_q, w_k, w_v, w_o
    )))


def solution(mesh):
    placed = (
        P(("batch", "seq"), "nbr"),
        P(("batch", "seq"), "nbr"),
        P(("batch", "seq", "nbr"), None, None),
        P(("batch", "seq")),
        P("nbr"),
        P(),
        P("nbr", None),
        P(),
        P("seq", "nbr"),
        P("seq", "nbr"),
        P("seq", "nbr"),
        P("nbr", "seq"),
    )
    return jax.shard_map(
        body,
        mesh=mesh,
        in_specs=placed,
        out_specs=(
            P(("batch", "seq"), "nbr"),
            P(("batch", "seq"), "nbr"),
            P(("batch", "seq", "nbr"), None, None),
            P(("batch", "nbr"), "seq"),
            P(("batch", "seq"), "nbr"),
            P(("batch", "seq"), "nbr"),
        ),
        check_vma=False,
    )
```

```python
import functools

import jax
import jax.numpy as jnp
from jax import lax
from jax.experimental import pallas as pl
from jax.experimental.pallas import tpu as pltpu
from jax.sharding import PartitionSpec as P

HD = 128
CLEN = 64
NLEN = 128
KMAX = 8
BF = jnp.bfloat16
F32 = jnp.float32
MESH = pl.DeviceIdType.MESH
ANY = pl.BlockSpec(memory_space=pl.ANY)
NT = (((1,), (1,)), ((), ()))
TN = (((0,), (0,)), ((), ()))
TILE = 256

dot = functools.partial(lax.dot_general, preferred_element_type=F32)


def mm(a, b):
    return jnp.dot(a, b, preferred_element_type=F32)


def remote(src, dst, send, recv, dev):
    return pltpu.make_async_remote_copy(
        src_ref=src, dst_ref=dst, send_sem=send, recv_sem=recv, device_id=dev, device_id_type=MESH
    )


def cols(ref, i, width):
    return ref.at[:, pl.ds(pl.multiple_of(i * width, 128), width)]


def rows_of(ref, i, count):
    return ref.at[pl.ds(pl.multiple_of(i * count, 8), count)]


def tiles(count, step, body):
    def one(t, _):
        body(pl.multiple_of(t * step, step))
        return 0

    lax.fori_loop(0, count // step, one, 0)


def layer_kernel(n_seq, n_nbr, names, *refs):
    hidden, d_out, gain, emb, span, w_cond, w_enc, w_q, w_k, w_v, w_o = refs[:11]
    out_o, dh_o, denc_o, dwo_o, dwk_o, dwv_o = refs[11:17]
    S = dict(zip(names, refs[17:]))
    hid, dout, gains, wq, wo, wkv = (S[k] for k in ("hid", "dout", "gains", "wq", "wo", "wkv"))
    enc, enct, kv, big, norm, rst = (S[k] for k in ("enc", "enct", "kv", "big", "norm", "rst"))
    prob, dsend, drecv = S["prob"], S["dsend"], S["drecv"]
    e1, e2, e3, po, pd = (S[k] for k in ("emb", "e2", "e3", "po", "pd"))
    ro, rd, q_s, da_s, dq_s = (S[k] for k in ("ro", "rd", "q", "da", "dq"))
    att, dcol, pw, wr, dwo, dwf = (S[k] for k in ("att", "dcol", "pw", "wr", "dwo", "dwf"))
    emb_v, cond_v, enc_v, pool = (S[k] for k in ("emb", "cond", "wenc", "pool"))
    cpart, crecv, st = (S[k] for k in ("cpart", "crecv", "st"))
    lsem, osem, zs, zr, ps, pr = (S[k] for k in ("lsem", "osem", "zs", "zr", "ps", "pr"))
    ns, nr, es, er, ss, sr = (S[k] for k in ("ns", "nr", "es", "er", "ss", "sr"))
    us, ur, ks, kr = (S[k] for k in ("us", "ur", "ks", "kr"))

    s, n, b = lax.axis_index("seq"), lax.axis_index("nbr"), lax.axis_index("batch")
    x, y, core, diag = {"nbr": n ^ 1}, {"nbr": n ^ 2}, {"batch": 1 - b}, {"nbr": n ^ 3}
    right, left = {"seq": s + 1}, {"seq": s - 1}
    has_right, has_left = s + 1 < n_seq, s > 0
    tokens, feat = hidden.shape
    spans = tokens // CLEN
    slots, width = emb.shape[0], emb.shape[2]
    total = slots * n_nbr
    local = w_q.shape[1]
    heads = local // HD
    half_slots = slots // 2
    unit = half_slots * NLEN
    wr_q, wr_k, piece = w_q.shape[0], w_k.shape[0], w_o.shape[1]

    own = {
        "h": cols(hid, n, feat), "d": cols(dout, n, feat), "g": gains.at[n],
        "k": rows_of(wkv, s, wr_k).at[:, pl.ds(0, local)],
        "v": rows_of(wkv, s, wr_k).at[:, pl.ds(local, local)],
        "q": rows_of(wq, s, wr_q), "o": cols(wo, s, piece),
    }
    source = {"h": hidden, "d": d_out, "g": gain.at[:, pl.ds(0, feat)], "k": w_k, "v": w_v, "q": w_q, "o": w_o}
    loads = {
        k: pltpu.make_async_copy(source[k], own[k], lsem.at[i]) for i, k in enumerate(("h", "d", "g", "k", "v", "q", "o"))
    }
    loads["c"] = pltpu.make_async_copy(w_cond, cond_v, lsem.at[7])
    loads["e"] = pltpu.make_async_copy(emb, emb_v, lsem.at[8])
    loads["w"] = pltpu.make_async_copy(w_enc, enc_v, lsem.at[9])
    loads["n"] = pltpu.make_async_copy(gain.at[:, pl.ds(feat, width)], S["egain"], lsem.at[10])
    for k in ("h", "k", "v", "q", "g", "c", "d", "e", "w", "n", "o"):
        loads[k].start()

    barrier = pltpu.get_barrier_semaphore()
    for dev in (x, y, diag, core):
        pl.semaphore_signal(barrier, inc=1, device_id=dev, device_id_type=MESH)
    for k in range(1, n_seq):
        pl.semaphore_signal(barrier, inc=1, device_id={"seq": lax.rem(s + k, n_seq)}, device_id_type=MESH)

    loads["h"].wait()
    means = []
    for c in range(spans):
        part = cols(hid, n, feat)[c * CLEN : (c + 1) * CLEN, :].astype(F32)
        means.append((jnp.sum(part, axis=0, keepdims=True) / CLEN).astype(BF).astype(F32))
    pool[0] = jnp.broadcast_to(means[spans - 1], pool.shape[1:])
    pl.semaphore_wait(barrier, n_seq + 3)

    def carry(dev):
        return remote(pool.at[0], pool.at[1], ss.at[0], sr.at[0], dev)

    @pl.when(has_right)
    def _():
        carry(right).start()

    order = ("k", "v", "q", "o")

    def block(a, j):
        if a == "k":
            return rows_of(wkv, j, wr_k).at[:, pl.ds(0, local)]
        if a == "v":
            return rows_of(wkv, j, wr_k).at[:, pl.ds(local, local)]
        if a == "q":
            return rows_of(wq, j, wr_q)
        return cols(wo, j, piece)

    def half(a, j, h):
        if a in ("k", "v"):
            w = local // 2
            base = 0 if a == "k" else local
            return rows_of(wkv, j, wr_k).at[:, pl.ds(pl.multiple_of(base + h * w, 128), w)]
        if a == "q":
            c = wr_q // 2
            return wq.at[pl.ds(pl.multiple_of(j * wr_q + h * c, 8), c)]
        c = local // 2
        return wo.at[pl.ds(pl.multiple_of(h * c, 8), c), pl.ds(pl.multiple_of(j * piece, 128), piece)]

    def ring(a, k, d):
        j = s - k + 1 if d == 0 else s + k - 1
        i = order.index(a)
        part = half(a, j, b)
        return remote(part, part, zs.at[i, k, d], zr.at[i, k, d], right if d == 0 else left)

    def guard(d, k):
        if d == 0:
            return has_right & (s - (k - 1) >= 0)
        return has_left & (s + (k - 1) < n_seq)

    def valid(d, k):
        return (s - k >= 0) if d == 0 else (s + k < n_seq)

    def launch(a, ready=False):
        if not ready:
            loads[a].wait()
        for d in (0, 1):
            @pl.when(guard(d, 1))
            def _(a=a, d=d):
                ring(a, 1, d).start()

    def share(a, k, d, h):
        j = s - k if d == 0 else s + k
        i = order.index(a)
        part = half(a, j, h)
        return remote(part, part, ps.at[i, k, d], pr.at[i, k, d], core)

    def relay(a, k, kind="all"):
        i = order.index(a)
        for d in (0, 1):
            onward = guard(d, k + 1) if k + 1 < n_seq else valid(d, k) & (s < 0)
            when = {"all": valid(d, k), "on": onward, "end": valid(d, k) & jnp.logical_not(onward)}[kind]

            @pl.when(when)
            def _(d=d):
                part = half(a, s - k if d == 0 else s + k, b)
                remote(part, part, zs.at[i, k, d], zr.at[i, k, d], left if d == 0 else right).wait_recv()
                share(a, k, d, b).start()

            if k + 1 < n_seq and kind != "end":
                @pl.when(guard(d, k + 1))
                def _(d=d):
                    ring(a, k + 1, d).start()

    def arrived(a):
        for k in range(1, n_seq):
            for d in (0, 1):
                @pl.when(valid(d, k))
                def _(k=k, d=d):
                    share(a, k, d, 1 - b).wait_recv()

    def wave(w, skip=()):
        for a, lag in (("k", 0), ("v", 0), ("q", 1)):
            if 1 <= w - lag < n_seq and a not in skip:
                relay(a, w - lag)

    for a in ("k", "v", "q"):
        launch(a)

    def pair(key, i):
        ref = own[key]
        return [remote(ref, ref, ns.at[i, d], nr.at[i, d], dev) for d, dev in enumerate((x, y))]

    for c in pair("h", 0):
        c.start()
    loads["g"].wait()
    gain_sends = [
        remote(own["g"], own["g"], ns.at[2, d], nr.at[2, d], dev) for d, dev in enumerate((x, y, diag))
    ]
    for c in gain_sends:
        c.start()

    @pl.when(has_left)
    def _():
        carry(left).wait_recv()

    @pl.when(jnp.logical_not(has_left))
    def _():
        pool[1] = jnp.zeros(pool.shape[1:], F32)

    place = lax.broadcasted_iota(jnp.int32, pool.shape[1:], 0)
    before = pool[1]
    for c in range(1, spans):
        before = jnp.where(place == c, jnp.broadcast_to(means[c - 1], before.shape), before)
    loads["c"].wait()
    cpart[...] = mm(before.astype(BF), cond_v[...])
    sums = [remote(cpart, crecv.at[d], ss.at[1 + d], sr.at[1 + d], dev) for d, dev in enumerate((x, y, diag))]
    for c in sums:
        c.start()
    loads["d"].wait()
    for c in pair("d", 1):
        c.start()
    for c in sums:
        c.wait_recv()
    condition = cpart[...] + crecv[0] + crecv[1] + crecv[2]

    def slot_rows(m, j):
        return pl.ds(pl.multiple_of((m * slots + j) * NLEN, NLEN), NLEN)

    def slot_copy(src, j, i, dev):
        part = enc.at[slot_rows(src, j)]
        return remote(part, part, es.at[j, i], er.at[j, i], dev)

    def diagonal(ref, i):
        c = tokens // 2
        for d, (src, dev) in enumerate(((n ^ 1, y), (n ^ 2, x))):
            full = cols(ref, src, feat)
            remote(full, full, ns.at[i, d], nr.at[i, d], dev).wait_recv()
            part = full.at[pl.ds(d * c, c)]
            remote(part, part, ns.at[i, 2 + d], nr.at[i, 2 + d], dev).start()

    diagonal(hid, 0)
    loads["e"].wait()
    loads["w"].wait()
    loads["n"].wait()
    gain_row = S["egain"][0:1].astype(F32)
    for j in range(slots):
        mark = jnp.full((1, width), span[n * slots + j], jnp.int32)
        vals = emb_v[j].astype(F32)
        for c in range(spans):
            vals = vals + jnp.where(mark == c, condition[c : c + 1], 0.0)
        scale = lax.rsqrt(jnp.mean(vals * vals, axis=-1, keepdims=True) + 1e-06)
        mixed = mm((vals * scale * gain_row).astype(BF), enc_v[...])
        enc[slot_rows(n, j), :] = (vals + mixed / (1.0 + jnp.exp(-mixed))).astype(BF)
        slot_copy(n, j, 0, x).start()
        slot_copy(n, j, 1, y).start()
        if j == 1:
            diagonal(dout, 1)
        if j == half_slots:
            wave(1)

    def diagonal_done(ref, i):
        c = tokens // 2
        for d in (0, 1):
            part = cols(ref, n ^ 3, feat).at[pl.ds(d * c, c)]
            remote(part, part, ns.at[i, 2 + d], nr.at[i, 2 + d], x).wait()

    def pass_on(j):
        for d, (src, dev) in enumerate(((n ^ 1, y), (n ^ 2, x))):
            slot_copy(src, j, d, dev).wait_recv()
            if j % 2 == d:
                slot_copy(src, j, 2, dev).start()

    def project(m, j):
        at = pl.multiple_of((m * slots + j) * NLEN, NLEN)
        slot = pl.ds(m * slots + j, half_slots)
        block_rows = enc[pl.ds(at, unit), :]
        enct[:, pl.ds(at, unit)] = block_rows.T

        def tile(c):
            res = mm(enc[pl.ds(at, unit), :], wkv[:, pl.ds(c, TILE)]).astype(BF)
            kv[slot, :, pl.ds(c, TILE)] = res.reshape(half_slots, NLEN, TILE)

        tiles(2 * local, TILE, tile)

    wave(2)
    diagonal_done(dout, 1)
    def z_sends():
        found = []
        for k in range(1, n_seq):
            peer = lax.rem(s + k, n_seq)
            found.append(remote(cols(dout, peer, piece), rows_of(dcol, s, tokens), ks.at[4, k], kr.at[4, k], {"seq": peer}))
        return found

    dcol_sends = z_sends()
    def edge(i):
        return (i == 0) | (i == n_seq - 1)

    def columns(late):
        for k in range(1, n_seq):
            delayed = edge(lax.rem(s + k, n_seq)) & jnp.logical_not(edge(s))

            @pl.when(delayed if late else jnp.logical_not(delayed))
            def _(k=k):
                dcol_sends[k - 1].start()

    columns(False)
    dcol[pl.ds(pl.multiple_of(s * tokens, tokens), tokens), :] = dout[:, pl.ds(pl.multiple_of(s * piece, 128), piece)]


    for j in range(half_slots):
        pass_on(j)
    diagonal_done(hid, 0)
    for c in gain_sends:
        c.wait_recv()

    def norm_rows(r):
        part = hid[pl.ds(r, 32), :].astype(F32)
        scale = lax.rsqrt(jnp.mean(part * part, axis=-1, keepdims=True) + 1e-06)
        rst[pl.ds(r, 32), :] = jnp.broadcast_to(scale, (32, HD))
        for m in range(n_nbr):
            vals = hid[pl.ds(r, 32), m * feat : (m + 1) * feat].astype(F32) * scale * gains[m, 0:1].astype(F32)
            norm[pl.ds(r, 32), m * feat : (m + 1) * feat] = vals.astype(BF)

    tiles(tokens, 32, norm_rows)
    wave(3)
    for w in range(4, n_seq):
        wave(w)
    for j in range(half_slots, slots):
        pass_on(j)
    arrived("k")
    arrived("v")
    for m in (n, n ^ 1, n ^ 2):
        project(m, 0)

    columns(True)
    loads["o"].wait()

    def da_copy(k):
        peer = lax.rem(s + n_seq - k, n_seq)
        return remote(dsend.at[k], drecv.at[k], ks.at[3, k], kr.at[3, k], {"seq": peer})

    def da_parts(late):
        for i in range(1, n_seq):
            k = i + (n_seq - 2 * i) * (s > 0).astype(jnp.int32)
            peer = lax.rem(s + n_seq - k, n_seq)
            delayed = edge(s) & jnp.logical_not(edge(peer))

            @pl.when(delayed if late else jnp.logical_not(delayed))
            def _(k=k, peer=peer):
                rows = rows_of(dcol, peer, tokens)
                remote(rows, rows, ks.at[4, k], kr.at[4, k], {"seq": peer}).wait_recv()
                part = dot(rows[...], wo[:, pl.ds(pl.multiple_of(s * piece, 128), piece)], NT)
                dsend[k] = part.astype(BF)
                da_copy(k).start()

    da_parts(False)
    wave(n_seq)
    for m in (n, n ^ 1, n ^ 2):
        project(m, half_slots)
    for j in range(slots):
        slot_copy(n ^ 3, j, 2, x).wait_recv()
        if (j + 1) % half_slots == 0:
            project(n ^ 3, j + 1 - half_slots)
    arrived("q")

    def query(c):
        q_s[:, pl.ds(c, TILE)] = mm(norm[...], wq[:, pl.ds(c, TILE)]).astype(BF)

    tiles(local, TILE, query)

    ids = [span[j] for j in range(total)]
    run = [jnp.int32(0)] * spans
    inv = []
    for j in range(total):
        at = jnp.int32(-1)
        for c in range(spans):
            hit = (ids[j] == c).astype(jnp.int32)
            at = at + hit * (c * KMAX + 1 + run[c])
            run[c] = run[c] + hit
        inv.append(at)
    for i in range(spans * KMAX):
        at = jnp.int32(0)
        for j in range(1, total):
            at = at + (inv[j] == i).astype(jnp.int32) * j
        big[i] = kv[at]

    keys = KMAX * NLEN
    factor = HD ** (-0.5)
    tok0 = pl.multiple_of(s * tokens, tokens)

    spot = lax.broadcasted_iota(jnp.int32, (1, keys), 1)
    bias = [jnp.where(spot < run[c] * NLEN, 0.0, -1e30) for c in range(spans)]

    def forward(h, _):
        hc = pl.ds(pl.multiple_of(h * HD, HD), HD)
        vc = pl.ds(pl.multiple_of(local + h * HD, HD), HD)
        for c in range(spans):
            kc = pl.ds(c * KMAX, KMAX)
            k, v = big[kc, :, hc].reshape(keys, HD), big[kc, :, vc].reshape(keys, HD)
            scores = dot(q_s[pl.ds(c * CLEN, CLEN), hc], k, NT) * factor + bias[c]
            weights = jnp.exp(scores - jnp.max(scores, axis=-1, keepdims=True))
            probs = weights * (1.0 / jnp.sum(weights, axis=-1, keepdims=True))
            prob[c, h] = probs
            att[pl.ds(pl.multiple_of(tok0 + c * CLEN, CLEN), CLEN), hc] = mm(probs.astype(BF), v).astype(BF)
        return 0

    lax.fori_loop(0, heads, forward, 0)
    da_parts(True)
    own_rows = dcol[pl.ds(tok0, tokens), :]
    acc = dot(own_rows, wo[:, pl.ds(pl.multiple_of(s * piece, 128), piece)], NT)
    for k in range(1, n_seq):
        da_copy(k).wait_recv()
        acc = acc + drecv[k].astype(F32)
    da_s[...] = acc.astype(BF)
    launch("o", True)

    def backward(h, _):
        hc = pl.ds(pl.multiple_of(h * HD, HD), HD)
        vc = pl.ds(pl.multiple_of(local + h * HD, HD), HD)
        for c in range(spans):
            tr, kc, gc = pl.ds(c * CLEN, CLEN), pl.ds(c * KMAX, KMAX), pl.ds((spans + c) * KMAX, KMAX)
            q, da, probs = q_s[tr, hc], da_s[tr, hc], prob[c, h]
            k, v = big[kc, :, hc].reshape(keys, HD), big[kc, :, vc].reshape(keys, HD)
            d_probs = dot(da, v, NT)
            row_dot = jnp.sum(probs * d_probs, axis=-1, keepdims=True)
            d_scores = (probs * (d_probs - row_dot) * factor).astype(BF)
            dq_s[tr, hc] = mm(d_scores, k).astype(BF)
            big[gc, :, hc] = dot(d_scores, q, TN).astype(BF).reshape(KMAX, NLEN, HD)
            big[gc, :, vc] = dot(probs.astype(BF), da, TN).astype(BF).reshape(KMAX, NLEN, HD)
        return 0

    lax.fori_loop(0, heads, backward, 0)

    att_own = rows_of(att, s, tokens)
    att_sends = [
        remote(att_own, att_own, ks.at[1, k], kr.at[1, k], {"seq": lax.rem(s + k, n_seq)}) for k in range(1, n_seq)
    ]
    for c in att_sends:
        c.start()

    for j in range(total):
        vals = big[spans * KMAX + jnp.clip(inv[j], 0, spans * KMAX - 1)]
        mark = jnp.full(vals.shape, inv[j], jnp.int32)
        kv[j] = jnp.where(mark >= 0, vals.astype(F32), 0.0).astype(BF)

    class Sum:
        def __init__(self, i, route, part, first, forward, last):
            self.i, self.part, self.r = i, part, (forward, first, last)
            self.near, self.far = (n ^ 1, n ^ 2) if route == 0 else (n ^ 2, n ^ 1)

        def copy(self, step):
            m = (n ^ 3, self.near, self.far)[step]
            dev = {"nbr": self.far if step == 2 else self.near}
            return remote(self.part(m), self.r[step], us.at[self.i, step], ur.at[self.i, step], dev)

        def second(self):
            self.copy(0).wait_recv()
            mine = self.part(self.far)
            mine[...] = (mine[...].astype(F32) + self.r[0][...].astype(F32)).astype(BF)
            self.copy(2).start()

        def result(self):
            self.copy(1).wait_recv()
            self.copy(2).wait_recv()
            return self.part(n)[...].astype(F32) + self.r[1][...].astype(F32) + self.r[2][...].astype(F32)

    enc_sums = [
        Sum(j, 0 if j < half_slots else 1, lambda m, j=j: big.at[m * slots + j, :, pl.ds(0, width)], e1.at[j], e2.at[j], e3.at[j])
        for j in range(slots)
    ]
    hr = tokens // 2
    out_sums = [
        Sum(slots + h, h, lambda m, h=h: po.at[m, pl.ds(h * hr, hr)], ro.at[0, h], ro.at[1, h], ro.at[2, h])
        for h in (0, 1)
    ]
    dn_sums = [
        Sum(slots + 2 + h, h, lambda m, h=h: pd.at[m, pl.ds(h * hr, hr)], rd.at[0, h], rd.at[1, h], rd.at[2, h])
        for h in (0, 1)
    ]

    def back(m, j):
        slot = pl.ds(m * slots + j, half_slots)
        vals = kv[slot].reshape(unit, 2 * local)
        for c in range(0, width, TILE):
            w = min(TILE, width - c)
            big[slot, :, c : c + w] = dot(vals, wkv[c : c + w, :], NT).astype(BF).reshape(half_slots, NLEN, w)

    sets = (range(0, half_slots), range(half_slots, slots))
    for h in (0, 1):
        back(n ^ 3, h * half_slots)
        for j in sets[h]:
            enc_sums[j].copy(0).start()

    def d_weights(c):
        pw[:, pl.ds(c, TILE)] = mm(enct[...], kv[:, :, pl.ds(c, TILE)].reshape(total * NLEN, TILE)).astype(BF)

    tiles(2 * local, TILE, d_weights)

    def w_copy(d, i):
        place = i if d == 0 else i + (n_seq - i) * (s - 1 == i).astype(jnp.int32)
        dev = right if d == 0 else left
        return remote(rows_of(pw, i, wr_k), wr.at[place], ks.at[d * 2, i], kr.at[d * 2, i], dev)

    def w_sends_on(d, i):
        return (s < i) if d == 0 else (s > i)

    w_steps = []
    for i in range(n_seq - 1):
        w_steps += [(0, n_seq - 1 - i), (1, i)]
    for d, i in w_steps:
        @pl.when(w_sends_on(d, i) & ((s == 0) if d == 0 else (s == n_seq - 1)))
        def _(d=d, i=i):
            w_copy(d, i).start()

    for h in (0, 1):
        back((n ^ 1, n ^ 2)[h], h * half_slots)
        for j in sets[h]:
            enc_sums[j].copy(1).start()
    relay("o", 1, "on")

    def out_part(m):
        def tile(c):
            wc = pl.ds(pl.multiple_of(m * feat + c, TILE), TILE)
            po[m, :, pl.ds(c, TILE)] = mm(att[pl.ds(tok0, tokens), :], wo[:, wc]).astype(BF)

        tiles(feat, TILE, tile)

    def dn_part(m):
        def tile(c):
            wc = pl.ds(pl.multiple_of(m * feat + c, TILE), TILE)
            pd[m, :, pl.ds(c, TILE)] = dot(dq_s[...], wq[wc, :], NT).astype(BF)

        tiles(feat, TILE, tile)

    def sum_parts(make, group):
        make(n ^ 3)
        for u in group:
            u.copy(0).start()
        make(n ^ 1)
        make(n ^ 2)
        for u in group:
            u.copy(1).start()
        make(n)

    sum_parts(dn_part, dn_sums)

    def stat_rows(r):
        acc = jnp.zeros((32, 1), F32)
        for m in range(n_nbr):
            vals = hid[pl.ds(r, 32), m * feat : (m + 1) * feat].astype(F32)
            grad = gains[m, 0:1].astype(F32) * pd[m, pl.ds(r, 32), :].astype(F32)
            acc = acc + jnp.sum(vals * grad, axis=-1, keepdims=True)
        rows = jnp.broadcast_to(acc / (n_nbr * feat), (32, HD))
        st[0, pl.ds(r, 32), :] = rows

    tiles(tokens, 32, stat_rows)
    st[4] = st[0].T
    stat_sends = [
        remote(st.at[4, pl.ds(0, 8)], st.at[1 + d, pl.ds(0, 8)], ss.at[4 + d], sr.at[4 + d], dev)
        for d, dev in enumerate((x, y, diag))
    ]
    for c in stat_sends:
        c.start()
    for k in range(2, n_seq):
        relay("o", k, "on")

    for h in (0, 1):
        back((n ^ 2, n ^ 1)[h], h * half_slots)
    for i in range(half_slots):
        enc_sums[i].second()
        enc_sums[half_slots + i].second()
    for d, i in w_steps:
        @pl.when(w_sends_on(d, i) & ((s > 0) if d == 0 else (s < n_seq - 1)))
        def _(d=d, i=i):
            w_copy(d, i).wait_recv()
            mine = rows_of(pw, i, wr_k)
            mine[...] = (mine[...].astype(F32) + wr[i].astype(F32)).astype(BF)
            w_copy(d, i).start()

    for k in range(1, n_seq):
        relay("o", k, "end")
    arrived("o")
    sum_parts(out_part, out_sums)
    for h in (0, 1):
        back(n, h * half_slots)
    for u in dn_sums + out_sums:
        u.second()

    writes = []

    def write(src, dst):
        c = pltpu.make_async_copy(src, dst, osem.at[len(writes)])
        c.start()
        writes.append(c)

    for c in att_sends:
        c.wait_recv()

    step = min(TILE, piece)

    def d_out_weights(c):
        dwo[:, pl.ds(c, step)] = dot(att[...], dcol[:, pl.ds(c, step)], TN)

    tiles(piece, step, d_out_weights)
    write(dwo, dwo_o)

    dwf[...] = rows_of(pw, s, wr_k)[...].astype(F32)

    @pl.when(has_left)
    def _():
        remote(wr.at[s], wr.at[s], ks.at[0, s], kr.at[0, s], left).wait_recv()
        dwf[...] = dwf[...] + wr[s].astype(F32)

    @pl.when(has_right)
    def _():
        remote(wr.at[n_seq], wr.at[n_seq], ks.at[2, s], kr.at[2, s], right).wait_recv()
        dwf[...] = dwf[...] + wr[n_seq].astype(F32)

    write(dwf.at[:, pl.ds(0, local)], dwk_o)
    write(dwf.at[:, pl.ds(local, local)], dwv_o)

    for i in range(half_slots):
        for j in (i, half_slots + i):
            e1[j] = enc_sums[j].result().astype(BF)
            write(e1.at[j], denc_o.at[j])
    for h, u in enumerate(out_sums):
        vals = cols(hid, n, feat)[h * hr : (h + 1) * hr, :].astype(F32)
        ro[0, h] = (vals + u.result()).astype(BF)
        write(ro.at[0, h], out_o.at[pl.ds(h * hr, hr)])
    for c in stat_sends:
        c.wait_recv()
    stat_row = st[4, 0:1] + st[1, 0:1] + st[2, 0:1] + st[3, 0:1]
    stat = jnp.broadcast_to(stat_row, (tokens, tokens)).T
    for h, u in enumerate(dn_sums):
        rr = slice(h * hr, (h + 1) * hr)
        vals = cols(hid, n, feat)[rr, :].astype(F32)
        grad = gains[n, 0:1].astype(F32) * u.result()
        scale = rst[rr, 0:1]
        res = cols(dout, n, feat)[rr, :].astype(F32) + scale * grad - vals * scale**3 * stat[rr, 0:1]
        rd[0, h] = res.astype(BF)
        write(rd.at[0, h], dh_o.at[pl.ds(h * hr, hr)])

    @pl.when(has_right)
    def _():
        carry(right).wait_send()

    for a in order:
        for k in range(1, n_seq):
            for d in (0, 1):
                @pl.when(valid(d, k))
                def _(a=a, k=k, d=d):
                    share(a, k, d, b).wait_send()

                @pl.when(guard(d, k))
                def _(a=a, k=k, d=d):
                    ring(a, k, d).wait_send()
    for c in pair("h", 0) + pair("d", 1) + gain_sends + sums + stat_sends + dcol_sends + [da_copy(k) for k in range(1, n_seq)] + att_sends:
        c.wait_send()
    for d, i in w_steps:
        @pl.when(w_sends_on(d, i))
        def _(d=d, i=i):
            w_copy(d, i).wait_send()

    for j in range(slots):
        for i in range(3):
            slot_copy(n, j, i, x).wait_send()
    for u in enc_sums + out_sums + dn_sums:
        for i in range(3):
            u.copy(i).wait_send()
    for c in writes:
        c.wait()


def layer(hidden, d_out, gain, emb, span, w_cond, w_enc, w_q, w_k, w_v, w_o):
    n_seq, n_nbr = lax.axis_size("seq"), lax.axis_size("nbr")
    args = (hidden, d_out, gain, emb, span, w_cond, w_enc, w_q, w_k, w_v, w_o)
    tokens, feat = hidden.shape
    slots, _, width = emb.shape
    total = slots * n_nbr
    local, piece, wr_k = w_q.shape[1], w_o.shape[1], w_k.shape[0]
    spans = tokens // CLEN
    full = feat * n_nbr
    vm = pltpu.VMEM
    dma = pltpu.SemaphoreType.DMA
    scratch = dict(
        hid=vm((tokens, full), BF), dout=vm((tokens, full), BF), gains=vm((n_nbr, gain.shape[0], feat), BF), egain=vm((gain.shape[0], width), BF),
        wq=vm((full, local), BF), wo=vm((local, full), BF), wkv=vm((width, 2 * local), BF),
        enc=vm((total * NLEN, width), BF), enct=vm((width, total * NLEN), BF),
        kv=vm((total, NLEN, 2 * local), BF), big=vm((2 * spans * KMAX, NLEN, 2 * local), BF),
        norm=vm((tokens, full), BF), prob=vm((spans, local // HD, CLEN, KMAX * NLEN), F32), rst=vm((tokens, HD), F32),
        e2=vm(emb.shape, BF), e3=vm(emb.shape, BF),
        po=vm((n_nbr, tokens, feat), BF), pd=vm((n_nbr, tokens, feat), BF),
        ro=vm((3, 2, tokens // 2, feat), BF), rd=vm((3, 2, tokens // 2, feat), BF),
        q=vm((tokens, local), BF), da=vm((tokens, local), BF), dq=vm((tokens, local), BF),
        att=vm((n_seq * tokens, local), BF), dcol=vm((n_seq * tokens, piece), BF),
        pw=vm((width, 2 * local), BF), wr=vm((n_seq + 1, wr_k, 2 * local), BF),
        dwo=vm((local, piece), F32), dwf=vm((wr_k, 2 * local), F32),
        emb=vm(emb.shape, BF), cond=vm(w_cond.shape, BF), wenc=vm(w_enc.shape, BF),
        pool=vm((2, 8, feat), F32), cpart=vm((8, width), F32), crecv=vm((3, 8, width), F32),
        st=vm((5, tokens, HD), F32),
        lsem=dma((11,)), osem=dma((slots + 8,)),
        zs=dma((4, n_seq, 2)), zr=dma((4, n_seq, 2)), ps=dma((4, n_seq, 2)), pr=dma((4, n_seq, 2)),
        ns=dma((3, 4)), nr=dma((3, 4)), es=dma((slots, 3)), er=dma((slots, 3)),
        ss=dma((7,)), sr=dma((7,)), us=dma((slots + 4, 3)), ur=dma((slots + 4, 3)),
        ks=dma((5, n_seq)), kr=dma((5, n_seq)),
        dsend=vm((n_seq, tokens, local), BF), drecv=vm((n_seq, tokens, local), BF),
    )
    specs = [ANY] * 11
    specs[4] = pl.BlockSpec(memory_space=pltpu.SMEM)
    shapes = [
        jax.ShapeDtypeStruct(hidden.shape, BF), jax.ShapeDtypeStruct(hidden.shape, BF),
        jax.ShapeDtypeStruct(emb.shape, BF), jax.ShapeDtypeStruct(w_o.shape, F32),
        jax.ShapeDtypeStruct(w_k.shape, F32), jax.ShapeDtypeStruct(w_v.shape, F32),
    ]
    return pl.pallas_call(
        functools.partial(layer_kernel, n_seq, n_nbr, tuple(scratch)),
        out_shape=shapes,
        in_specs=specs,
        out_specs=[ANY] * 6,
        scratch_shapes=list(scratch.values()),
        compiler_params=pltpu.CompilerParams(
            collective_id=0, has_side_effects=True, vmem_limit_bytes=67043328
        ),
        name="layer",
    )(*args)


def settle_kernel(*refs):
    count = len(refs) // 3
    ins, outs, bufs = refs[:count], refs[count : 2 * count], refs[2 * count : 3 * count]
    sems = refs[3 * count]
    loads = [pltpu.make_async_copy(a, v, sems.at[0, i]) for i, (a, v) in enumerate(zip(ins, bufs))]
    stores = [pltpu.make_async_copy(v, o, sems.at[1, i]) for i, (v, o) in enumerate(zip(bufs, outs))]
    for c in loads:
        c.start()
    for a, c in zip(loads, stores):
        a.wait()
        c.start()
    for c in stores:
        c.wait()


def settle(*arrays):
    count = len(arrays)
    return pl.pallas_call(
        settle_kernel,
        out_shape=[jax.ShapeDtypeStruct(v.shape, v.dtype) for v in arrays],
        in_specs=[ANY] * count,
        out_specs=[ANY] * count,
        scratch_shapes=[pltpu.VMEM(v.shape, v.dtype) for v in arrays] + [pltpu.SemaphoreType.DMA((2, count))],
        compiler_params=pltpu.CompilerParams(vmem_limit_bytes=60 * 2**20),
        name="settle",
    )(*arrays)


def body(hidden, d_out, nbr_emb, slot_span, dec_gain, enc_gain, w_cond, w_enc, w_q, w_k, w_v, w_o):
    both = jnp.concatenate([dec_gain, enc_gain])
    gain = jnp.broadcast_to(both[None], (16, both.shape[0]))
    return tuple(settle(*layer(
        hidden, d_out, gain, nbr_emb, slot_span, w_cond, w_enc, w_q, w_k, w_v, w_o
    )))


def solution(mesh):
    placed = (
        P(("batch", "seq"), "nbr"),
        P(("batch", "seq"), "nbr"),
        P(("batch", "seq", "nbr"), None, None),
        P(("batch", "seq")),
        P("nbr"),
        P(),
        P("nbr", None),
        P(),
        P("seq", "nbr"),
        P("seq", "nbr"),
        P("seq", "nbr"),
        P("nbr", "seq"),
    )
    return jax.shard_map(
        body,
        mesh=mesh,
        in_specs=placed,
        out_specs=(
            P(("batch", "seq"), "nbr"),
            P(("batch", "seq"), "nbr"),
            P(("batch", "seq", "nbr"), None, None),
            P(("batch", "nbr"), "seq"),
            P(("batch", "seq"), "nbr"),
            P(("batch", "seq"), "nbr"),
        ),
        check_vma=False,
    )
```
